32 devices in a mesh: dp: 2 (over z, core), tp: 16 (over x, y).
Axes of the slice: x: 4, y: 4, z: 1, core: 2. Of those that a mesh axis runs over, the one named last changes fastest.
The devices are a block of a 4x4x8 slice.
Arguments:
- x: bfloat16 [5120, 7168], P(('dp', 'tp')), parts along dimension 0
- dy: bfloat16 [5120, 7168], P(('dp', 'tp')), parts along dimension 0
- gate: bfloat16 [5120, 20480], P('dp', 'tp'), parts along dimension 0
- up: bfloat16 [5120, 20480], P('dp', 'tp'), parts along dimension 0
- w_gate: bfloat16 [7168, 20480], P(None, 'tp')
- w_up: bfloat16 [7168, 20480], P(None, 'tp')
- w_down: bfloat16 [20480, 7168], P('tp')
Outputs:
- output 1: bfloat16 [5120, 7168], P(('dp', 'tp')), parts along dimension 0
- output 2: bfloat16 [14336, 20480], P('dp', 'tp'), parts along dimension 0
- output 3: bfloat16 [14336, 20480], P('dp', 'tp'), parts along dimension 0
- output 4: bfloat16 [40960, 7168], P(('dp', 'tp')), parts along dimension 0
There are 2 independent parts. The reference program is written for one: setup_inputs(seed, part) draws one part's arguments, and reference() takes and returns one part's arrays. A program takes and returns all parts, laid end to end along the dimension named above; an argument that names none is the same for every part.
All inputs are finite; a program needn't handle non-finite values.
Results may differ from the reference program's by a relative error of at most 0.012.
Values are sent between devices in bfloat16 or wider.
A program may use at most 768 MiB of HBM per device.

```python
import jax
import jax.numpy as jnp

ROWS = 2560
D = 7168
FF = 20480


def act(gate, up):
    return jax.nn.silu(gate) * up


def setup_inputs(seed: int = 0, part: int = 0) -> dict:
    kx, ky, ka, kb, kg, ku, kd = jax.random.split(jax.random.key(seed), 7)
    kx, ky, ka, kb = (jax.random.fold_in(k, part) for k in (kx, ky, ka, kb))
    drawn = {
        "x": jax.random.normal(kx, (ROWS, D), jnp.float32),
        "dy": jax.random.normal(ky, (ROWS, D), jnp.float32),
        "gate": jax.random.normal(ka, (ROWS, FF), jnp.float32),
        "up": jax.random.normal(kb, (ROWS, FF), jnp.float32),
        "w_gate": jax.random.normal(kg, (D, FF), jnp.float32) * D**-0.5,
        "w_up": jax.random.normal(ku, (D, FF), jnp.float32) * D**-0.5,
        "w_down": jax.random.normal(kd, (FF, D), jnp.float32) * FF**-0.5,
    }
    return {k: v.astype(jnp.bfloat16) for k, v in drawn.items()}


def reference(x, dy, gate, up, w_gate, w_up, w_down):
    hidden, back = jax.vjp(act, gate.astype(jnp.float32), up.astype(jnp.float32))
    d_hidden = jnp.dot(dy, w_down.T, preferred_element_type=jnp.float32)
    d_gate, d_up = (g.astype(jnp.bfloat16) for g in back(d_hidden))
    dx = jnp.dot(d_gate, w_gate.T, preferred_element_type=jnp.float32) + jnp.dot(d_up, w_up.T, preferred_element_type=jnp.float32)
    dw_gate = jnp.dot(x.T, d_gate, preferred_element_type=jnp.float32)
    dw_up = jnp.dot(x.T, d_up, preferred_element_type=jnp.float32)
    dw_down = jnp.dot(hidden.astype(jnp.bfloat16).T, dy, preferred_element_type=jnp.float32)
    return tuple(g.astype(jnp.bfloat16) for g in (dx, dw_gate, dw_up, dw_down))
```

```python
import functools
import math

import jax
import jax.numpy as jnp
from jax import lax
from jax.experimental import pallas as pl
from jax.experimental.pallas import tpu as pltpu
from jax.sharding import PartitionSpec as P

MESH = pl.DeviceIdType.MESH
LINKS = ((0, 1), (0, -1), (1, 1), (1, -1))
TICKS = 3
FIRST = 3


def tile_of(size, want):
    return want if size % want == 0 else size


def gather_kernel(
    side, dt, nt,
    x_ref, dy_ref, gate_ref, up_ref, wg_ref, wu_ref, wd_ref,
    full_ref, dgu_ref, hid_ref, dxp_ref,
    wd_v, dy_v, g_v, u_v, dg_v, du_v, h_v, wg_t, wu_t, out_t,
    send_sem, recv_sem, wd_sem, in_sem, res_sem, w_sem, out_sem,
):
    rows, d = dy_ref.shape
    ff = gate_ref.shape[1]
    half, cols = rows // 2, d // 2
    ring = side - 1
    slots = side * side - 1
    me = lax.axis_index("tp")
    at = (me // side, me % side)

    def owner(da, db):
        return lax.rem(at[0] + da + 2 * side, side) * side + lax.rem(at[1] + db + 2 * side, side)

    def on_link(link, along, across):
        axis, sign = link
        steps = (sign * along, sign * across)
        return owner(*(steps if axis == 0 else steps[::-1]))

    def unit(link, slot, back):
        array, s = slot // slots, slot % slots
        early = s < 2 * ring
        late = jnp.maximum(s - 2 * ring, 0)
        hop = jnp.where(early, s // 2, late // ring) + 1
        across = jnp.where(early, 0, late % ring + 1)
        second = jnp.where(early, s % 2, 1)
        who = on_link(link, back - hop, -across)
        axis, sign = link
        col = second if axis == 0 else 1 - second
        row = pl.multiple_of(who * rows + (0 if sign == 1 else half), 8)
        return full_ref.at[array, pl.ds(row, half), pl.ds(pl.multiple_of(col * cols, 128), cols)]

    def copy(k, slot, src, dst):
        axis, sign = LINKS[k]
        return pltpu.make_async_remote_copy(
            src_ref=src,
            dst_ref=dst,
            send_sem=send_sem.at[k, slot],
            recv_sem=recv_sem.at[k, slot],
            device_id={"tp": on_link(LINKS[k], 1, 0)},
            device_id_type=MESH,
        )

    def send(slot):
        for k, link in enumerate(LINKS):
            part = unit(link, slot, 1)
            copy(k, slot, part, part).start()

    def arrive(slot):
        for k, link in enumerate(LINKS):
            part = unit(link, slot, 0)
            copy(k, slot, part, part).wait_recv()

    def step(slot):
        arrive(slot)

        @pl.when(slot + 2 < 2 * slots)
        def _():
            send(slot + 2)

    barrier = pltpu.get_barrier_semaphore()
    for link in LINKS:
        pl.semaphore_signal(barrier, inc=1, device_id={"tp": on_link(link, 1, 0)}, device_id_type=MESH)
    pl.semaphore_wait(barrier, len(LINKS))

    for slot in range(2):
        for k, (axis, sign) in enumerate(LINKS):
            col = slot if axis == 0 else 1 - slot
            r = 0 if sign == 1 else half
            part = (pl.ds(r, half), pl.ds(col * cols, cols))
            row = pl.multiple_of(me * rows + r, 8)
            copy(k, slot, dy_ref.at[part], full_ref.at[0, pl.ds(row, half), part[1]]).start()

    wd_copy = pltpu.make_async_copy(wd_ref, wd_v, wd_sem)
    wd_copy.start()

    mine = pl.ds(pl.multiple_of(me * rows, 8), rows)
    own = [dy_v.at[pl.ds(i * rows, rows)] for i in range(2)]
    loads = [pltpu.make_async_copy(ref, own[i], in_sem.at[0, i]) for i, ref in enumerate((dy_ref, x_ref))]
    stores = [pltpu.make_async_copy(own[i], full_ref.at[i, mine], in_sem.at[1, i]) for i in range(2)]
    for load in loads:
        load.start()
    for load, store in zip(loads, stores):
        load.wait()
        store.start()
    for store in stores:
        store.wait()

    tiles = d // dt

    def weights(i, slot):
        part = pl.ds(pl.multiple_of(i * dt, dt), dt)
        return [
            pltpu.make_async_copy(ref.at[part], buf.at[slot], w_sem.at[j, slot])
            for j, (ref, buf) in enumerate(((wg_ref, wg_t), (wu_ref, wu_t)))
        ]

    for c in weights(0, 0):
        c.start()
    lax.fori_loop(0, FIRST, lambda s, _: (step(s), None)[1], None)
    wd_copy.wait()

    groups = side * side // 2

    def group(g, _):
        starts = []
        for i in range(2):
            e = 2 * g + i
            a, b = e % side, e // side
            starts += [owner(-a, -b) * rows, owner(a, b) * rows + half]
        starts = [pl.multiple_of(s, 8) for s in starts]
        local = [pl.ds(i * half, half) for i in range(4)]
        there = [pl.ds(s, half) for s in starts]

        step(FIRST + TICKS * g)
        reads = [
            pltpu.make_async_copy(ref.at[t], buf.at[h], in_sem.at[j, i])
            for j, (ref, buf) in enumerate(((full_ref.at[0], dy_v), (gate_ref, g_v), (up_ref, u_v)))
            for i, (t, h) in enumerate(zip(there, local))
        ]
        for c in reads:
            c.start()
        for c in reads:
            c.wait()

        def hidden_tile(i, _):
            n = pl.ds(pl.multiple_of(i * nt, nt), nt)
            d_hidden = lax.dot_general(
                dy_v[...], wd_v[n, :], (((1,), (1,)), ((), ())), preferred_element_type=jnp.float32
            )
            gate, up = g_v[:, n].astype(jnp.float32), u_v[:, n].astype(jnp.float32)
            s = jax.nn.sigmoid(gate)
            silu = gate * s
            d_silu = d_hidden * up
            dg_v[:, n] = (d_silu * s + d_silu * gate * (s * (1 - s))).astype(dg_v.dtype)
            du_v[:, n] = (d_hidden * silu).astype(du_v.dtype)
            h_v[:, n] = (silu * up).astype(h_v.dtype)

        lax.fori_loop(0, ff // nt, hidden_tile, None)
        results = [
            pltpu.make_async_copy(buf.at[h], ref.at[t, c], res_sem.at[j, i])
            for j, (buf, ref, c) in enumerate((
                (dg_v, dgu_ref, pl.ds(0, ff)), (du_v, dgu_ref, pl.ds(ff, ff)), (h_v, hid_ref, pl.ds(0, ff)),
            ))
            for i, (t, h) in enumerate(zip(there, local))
        ]
        for c in results:
            c.start()

        def stores_of(i, slot):
            n = pl.ds(pl.multiple_of(i * dt, dt), dt)
            return [
                pltpu.make_async_copy(out_t.at[slot, h], dxp_ref.at[t, n], out_sem.at[slot, j])
                for j, (t, h) in enumerate(zip(there, local))
            ]

        def dx_tile(i, _):
            slot = i % 2
            for c in weights(i, slot):
                c.wait()

            @pl.when((i + 1 < tiles) | (g + 1 < groups))
            def _():
                for c in weights((i + 1) % tiles, (i + 1) % 2):
                    c.start()

            @pl.when(i >= 2)
            def _():
                for c in stores_of(i - 2, slot):
                    c.wait()

            nt_dims = (((1,), (1,)), ((), ()))
            term = lax.dot_general(dg_v[...], wg_t[slot], nt_dims, preferred_element_type=jnp.float32)
            term += lax.dot_general(du_v[...], wu_t[slot], nt_dims, preferred_element_type=jnp.float32)
            out_t[slot] = term.astype(out_t.dtype)
            for c in stores_of(i, slot):
                c.start()

        cut = (tiles // 2, tiles)
        step(FIRST + TICKS * g + 1)
        lax.fori_loop(0, cut[0], dx_tile, None)
        step(FIRST + TICKS * g + 2)
        lax.fori_loop(cut[0], cut[1], dx_tile, None)
        for i in (tiles - 2, tiles - 1):
            for c in stores_of(i, i % 2):
                c.wait()
        for c in results:
            c.wait()

    lax.fori_loop(0, groups, group, None)
    lax.fori_loop(FIRST + TICKS * groups, 2 * slots, lambda s, _: (step(s), None)[1], None)

    def sent(slot, _):
        for k, link in enumerate(LINKS):
            part = unit(link, slot, 1)
            copy(k, slot, part, part).wait_send()

    lax.fori_loop(0, 2 * slots, sent, None)


def gather(side, x, dy, gate, up, wg, wu, wd):
    rows, d = dy.shape
    tokens, ff = gate.shape
    n = side * side
    group = 2 * rows
    dt, nt = tile_of(d, 512), tile_of(ff, 256)
    bf16 = jnp.bfloat16
    flops = 6 * tokens * d * ff
    anywhere = pl.BlockSpec(memory_space=pl.ANY)
    return pl.pallas_call(
        functools.partial(gather_kernel, side, dt, nt),
        out_shape=(
            jax.ShapeDtypeStruct((2, tokens, d), bf16),
            jax.ShapeDtypeStruct((tokens, 2 * ff), bf16),
            jax.ShapeDtypeStruct((tokens, ff), bf16),
            jax.ShapeDtypeStruct((tokens, d), bf16),
        ),
        in_specs=[anywhere] * 7,
        out_specs=(anywhere,) * 4,
        scratch_shapes=[
            pltpu.VMEM((ff, d), bf16),
            pltpu.VMEM((group, d), bf16),
            *[pltpu.VMEM((group, ff), bf16)] * 5,
            *[pltpu.VMEM((2, dt, ff), bf16)] * 2,
            pltpu.VMEM((2, group, dt), bf16),
            pltpu.SemaphoreType.DMA((len(LINKS), 2 * (n - 1))),
            pltpu.SemaphoreType.DMA((len(LINKS), 2 * (n - 1))),
            pltpu.SemaphoreType.DMA,
            pltpu.SemaphoreType.DMA((3, 4)),
            pltpu.SemaphoreType.DMA((3, 4)),
            pltpu.SemaphoreType.DMA((2, 2)),
            pltpu.SemaphoreType.DMA((2, 4)),
        ],
        compiler_params=pltpu.CompilerParams(
            collective_id=0, has_side_effects=True, vmem_limit_bytes=60 * 1024 * 1024
        ),
        cost_estimate=pl.CostEstimate(
            flops=flops, bytes_accessed=2 * (8 * 2 * d * ff + 6 * tokens * d), transcendentals=tokens * ff
        ),
        name="gather_and_dx",
    )(x, dy, gate, up, wg, wu, wd)


def dw_in_kernel(x_ref, d_ref, dwg_ref, dwu_ref):
    ff = dwg_ref.shape[1]
    dw = lax.dot_general(
        x_ref[...], d_ref[...], (((0,), (0,)), ((), ())), preferred_element_type=jnp.float32
    )
    dwg_ref[...] = dw[:, :ff].astype(dwg_ref.dtype)
    dwu_ref[...] = dw[:, ff:].astype(dwu_ref.dtype)


def dw_in(full, dgu):
    _, tokens, d = full.shape
    ff = dgu.shape[1] // 2
    bd = tile_of(d, 256)
    out = jax.ShapeDtypeStruct((d, ff), full.dtype)
    return pl.pallas_call(
        dw_in_kernel,
        grid=(d // bd,),
        out_shape=(out, out),
        in_specs=[
            pl.BlockSpec((pl.squeezed, tokens, bd), lambda i: (1, 0, i)),
            pl.BlockSpec((tokens, 2 * ff), lambda i: (0, 0), pipeline_mode=pl.Buffered(1)),
        ],
        out_specs=[pl.BlockSpec((bd, ff), lambda i: (i, 0))] * 2,
        compiler_params=pltpu.CompilerParams(vmem_limit_bytes=60 * 1024 * 1024),
        cost_estimate=pl.CostEstimate(
            flops=4 * tokens * d * ff, bytes_accessed=2 * (tokens * d + 2 * ff * (tokens + d)), transcendentals=0
        ),
        name="dw_in",
    )(full, dgu)


def dw_out_kernel(h_ref, dy_ref, dw_ref, ht):
    @pl.when(pl.program_id(0) == 0)
    def _():
        ht[...] = h_ref[...].T

    dw = jnp.dot(ht[...], dy_ref[...], preferred_element_type=jnp.float32)
    dw_ref[...] = dw.astype(dw_ref.dtype)


def dw_out(full, hidden):
    _, tokens, d = full.shape
    ff = hidden.shape[1]
    bd = tile_of(d, 512)
    return pl.pallas_call(
        dw_out_kernel,
        grid=(d // bd,),
        out_shape=jax.ShapeDtypeStruct((ff, d), full.dtype),
        in_specs=[
            pl.BlockSpec((tokens, ff), lambda i: (0, 0), pipeline_mode=pl.Buffered(1)),
            pl.BlockSpec((pl.squeezed, tokens, bd), lambda i: (0, 0, i)),
        ],
        out_specs=pl.BlockSpec((ff, bd), lambda i: (0, i)),
        scratch_shapes=[pltpu.VMEM((ff, tokens), full.dtype)],
        compiler_params=pltpu.CompilerParams(vmem_limit_bytes=60 * 1024 * 1024),
        cost_estimate=pl.CostEstimate(
            flops=2 * tokens * d * ff, bytes_accessed=2 * (tokens * d + ff * (tokens + d)), transcendentals=0
        ),
        name="dw_out",
    )(hidden, full)


def solution(mesh):
    side = math.isqrt(mesh.shape["tp"])

    def device_step(x, dy, gate, up, w_gate, w_up, w_down):
        full, dgu, hidden, dx_terms = gather(side, x, dy, gate, up, w_gate, w_up, w_down)
        dx = lax.psum_scatter(dx_terms, "tp", scatter_dimension=0, tiled=True)
        dw_gate, dw_up = dw_in(full, dgu)
        dw_down = dw_out(full, hidden)
        return dx, dw_gate, dw_up, dw_down

    rows, both, cols = P(("dp", "tp"), None), P("dp", "tp"), P(None, "tp")
    return jax.shard_map(
        device_step,
        mesh=mesh,
        in_specs=(rows, rows, both, both, cols, cols, P("tp", None)),
        out_specs=(rows, both, both, rows),
        check_vma=False,
    )
```

```python
import functools
import math

import jax
import jax.numpy as jnp
from jax import lax
from jax.experimental import pallas as pl
from jax.experimental.pallas import tpu as pltpu
from jax.sharding import PartitionSpec as P

MESH = pl.DeviceIdType.MESH
LINKS = ((0, 1), (0, -1), (1, 1), (1, -1))
TICKS = 3
FIRST = 3


def tile_of(size, want):
    return want if size % want == 0 else size


def gather_kernel(
    side, dt, nt,
    x_ref, dy_ref, gate_ref, up_ref, wg_ref, wu_ref, wd_ref,
    full_ref, dgu_ref, hid_ref, *rest,
):
    terms, scratch = rest[: 4 * side], rest[4 * side :]
    (
    wd_v, dy_v, g_v, u_v, dg_v, du_v, h_v, wg_t, wu_t, out_t,
    send_sem, recv_sem, wd_sem, in_sem, res_sem, w_sem, out_sem,
    ) = scratch
    rows, d = dy_ref.shape
    ff = gate_ref.shape[1]
    half, cols = rows // 2, d // 2
    ring = side - 1
    slots = side * side - 1
    me = lax.axis_index("tp")
    at = (me // side, me % side)

    def owner(da, db):
        return lax.rem(at[0] + da + 2 * side, side) * side + lax.rem(at[1] + db + 2 * side, side)

    def on_link(link, along, across):
        axis, sign = link
        steps = (sign * along, sign * across)
        return owner(*(steps if axis == 0 else steps[::-1]))

    def unit(link, slot, back):
        array, s = slot // slots, slot % slots
        early = s < 2 * ring
        late = jnp.maximum(s - 2 * ring, 0)
        hop = jnp.where(early, s // 2, late // ring) + 1
        across = jnp.where(early, 0, late % ring + 1)
        second = jnp.where(early, s % 2, 1)
        who = on_link(link, back - hop, -across)
        axis, sign = link
        col = second if axis == 0 else 1 - second
        row = pl.multiple_of(who * rows + (0 if sign == 1 else half), 8)
        return full_ref.at[array, pl.ds(row, half), pl.ds(pl.multiple_of(col * cols, 128), cols)]

    def copy(k, slot, src, dst):
        axis, sign = LINKS[k]
        return pltpu.make_async_remote_copy(
            src_ref=src,
            dst_ref=dst,
            send_sem=send_sem.at[k, slot],
            recv_sem=recv_sem.at[k, slot],
            device_id={"tp": on_link(LINKS[k], 1, 0)},
            device_id_type=MESH,
        )

    def send(slot):
        for k, link in enumerate(LINKS):
            part = unit(link, slot, 1)
            copy(k, slot, part, part).start()

    def arrive(slot):
        for k, link in enumerate(LINKS):
            part = unit(link, slot, 0)
            copy(k, slot, part, part).wait_recv()

    def step(slot):
        arrive(slot)

        @pl.when(slot + 2 < 2 * slots)
        def _():
            send(slot + 2)

    barrier = pltpu.get_barrier_semaphore()
    for link in LINKS:
        pl.semaphore_signal(barrier, inc=1, device_id={"tp": on_link(link, 1, 0)}, device_id_type=MESH)
    pl.semaphore_wait(barrier, len(LINKS))

    for slot in range(2):
        for k, (axis, sign) in enumerate(LINKS):
            col = slot if axis == 0 else 1 - slot
            r = 0 if sign == 1 else half
            part = (pl.ds(r, half), pl.ds(col * cols, cols))
            row = pl.multiple_of(me * rows + r, 8)
            copy(k, slot, dy_ref.at[part], full_ref.at[0, pl.ds(row, half), part[1]]).start()

    wd_copy = pltpu.make_async_copy(wd_ref, wd_v, wd_sem)
    wd_copy.start()

    mine = pl.ds(pl.multiple_of(me * rows, 8), rows)
    own = [dy_v.at[pl.ds(i * rows, rows)] for i in range(2)]
    loads = [pltpu.make_async_copy(ref, own[i], in_sem.at[0, i]) for i, ref in enumerate((dy_ref, x_ref))]
    stores = [pltpu.make_async_copy(own[i], full_ref.at[i, mine], in_sem.at[1, i]) for i in range(2)]
    for load in loads:
        load.start()
    for load, store in zip(loads, stores):
        load.wait()
        store.start()
    for store in stores:
        store.wait()

    tiles = d // dt
    cut = tiles // 2

    def weights(i, slot):
        part = pl.ds(pl.multiple_of(i * dt, dt), dt)
        return [
            pltpu.make_async_copy(ref.at[part], buf.at[slot], w_sem.at[j, slot])
            for j, (ref, buf) in enumerate(((wg_ref, wg_t), (wu_ref, wu_t)))
        ]

    for c in weights(0, 0):
        c.start()
    lax.fori_loop(0, FIRST, lambda s, _: (step(s), None)[1], None)
    wd_copy.wait()

    def group(q, p):
        offsets = [2 * p, 2 * p + 1]
        starts = []
        for a in offsets:
            starts += [owner(-a, -q) * rows, owner(a, q) * rows + half]
        local = [pl.ds(i * half, half) for i in range(4)]
        there = [pl.ds(pl.multiple_of(s, 8), half) for s in starts]
        first = FIRST + TICKS * (q * (side // 2) + p)

        step(first)
        reads = [
            pltpu.make_async_copy(ref.at[t], buf.at[h], in_sem.at[j, i])
            for j, (ref, buf) in enumerate(((full_ref.at[0], dy_v), (gate_ref, g_v), (up_ref, u_v)))
            for i, (t, h) in enumerate(zip(there, local))
        ]
        for c in reads:
            c.start()
        for c in reads:
            c.wait()

        def hidden_tile(i, _):
            n = pl.ds(pl.multiple_of(i * nt, nt), nt)
            d_hidden = lax.dot_general(
                dy_v[...], wd_v[n, :], (((1,), (1,)), ((), ())), preferred_element_type=jnp.float32
            )
            gate, up = g_v[:, n].astype(jnp.float32), u_v[:, n].astype(jnp.float32)
            s = jax.nn.sigmoid(gate)
            silu = gate * s
            d_silu = d_hidden * up
            dg_v[:, n] = (d_silu * s + d_silu * gate * (s * (1 - s))).astype(dg_v.dtype)
            du_v[:, n] = (d_hidden * silu).astype(du_v.dtype)
            h_v[:, n] = (silu * up).astype(h_v.dtype)

        lax.fori_loop(0, ff // nt, hidden_tile, None)
        results = [
            pltpu.make_async_copy(buf.at[h], ref.at[t, c], res_sem.at[j, i])
            for j, (buf, ref, c) in enumerate((
                (dg_v, dgu_ref, pl.ds(0, ff)), (du_v, dgu_ref, pl.ds(ff, ff)), (h_v, hid_ref, pl.ds(0, ff)),
            ))
            for i, (t, h) in enumerate(zip(there, local))
        ]
        for c in results:
            c.start()

        def stores_of(i, slot, second, b):
            n = pl.ds(pl.multiple_of((i - second * cut) * dt, dt), dt)
            copies = []
            for j, a in enumerate(offsets):
                for r in range(2):
                    da, db = ((-a) % side, (side - b) % side) if r == 0 else (a, b)
                    key, at_ = (2 * side + 2 * db + r, da) if second else (2 * da + r, db)
                    k = 2 * j + r
                    copies.append(pltpu.make_async_copy(
                        out_t.at[slot, local[k]], terms[key].at[at_, :, n], out_sem.at[slot, k]
                    ))
            return copies

        def for_stores(i, slot, second, act):
            if not second:
                for c in stores_of(i, slot, second, q):
                    act(c)
                return
            for b in range(side):

                @pl.when(q == b)
                def _():
                    for c in stores_of(i, slot, second, b):
                        act(c)

        def dx_tile(second):
            begin = cut if second else 0

            def body(i, _):
                slot = i % 2
                for c in weights(i, slot):
                    c.wait()

                @pl.when((i + 1 < tiles) | (q + 1 < side) | (p + 1 < side // 2))
                def _():
                    for c in weights((i + 1) % tiles, (i + 1) % 2):
                        c.start()

                @pl.when(i >= begin + 2)
                def _():
                    for_stores(i - 2, slot, second, lambda c: c.wait())

                nt_dims = (((1,), (1,)), ((), ()))
                term = lax.dot_general(dg_v[...], wg_t[slot], nt_dims, preferred_element_type=jnp.float32)
                term += lax.dot_general(du_v[...], wu_t[slot], nt_dims, preferred_element_type=jnp.float32)
                out_t[slot] = term.astype(out_t.dtype)
                for_stores(i, slot, second, lambda c: c.start())

            end = tiles if second else cut
            lax.fori_loop(begin, end, body, None)
            for i in range(max(begin, end - 2), end):
                for_stores(i, i % 2, second, lambda c: c.wait())

        step(first + 1)
        dx_tile(False)
        step(first + 2)
        dx_tile(True)
        for c in results:
            c.wait()

    def groups(q, _):
        for p in range(side // 2):
            group(q, p)

    lax.fori_loop(0, side, groups, None)
    done = FIRST + TICKS * side * (side // 2)
    lax.fori_loop(done, 2 * slots, lambda s, _: (step(s), None)[1], None)

    def sent(slot, _):
        for k, link in enumerate(LINKS):
            part = unit(link, slot, 1)
            copy(k, slot, part, part).wait_send()

    lax.fori_loop(0, 2 * slots, sent, None)


def gather(side, x, dy, gate, up, wg, wu, wd):
    rows, d = dy.shape
    tokens, ff = gate.shape
    n = side * side
    group = 2 * rows
    dt, nt = tile_of(d // 2, 512), tile_of(ff, 256)
    bf16 = jnp.bfloat16
    flops = 6 * tokens * d * ff
    anywhere = pl.BlockSpec(memory_space=pl.ANY)
    return pl.pallas_call(
        functools.partial(gather_kernel, side, dt, nt),
        out_shape=(
            jax.ShapeDtypeStruct((2, tokens, d), bf16),
            jax.ShapeDtypeStruct((tokens, 2 * ff), bf16),
            jax.ShapeDtypeStruct((tokens, ff), bf16),
            *[jax.ShapeDtypeStruct((side, rows // 2, d // 2), bf16)] * (4 * side),
        ),
        in_specs=[anywhere] * 7,
        out_specs=(anywhere,) * (3 + 4 * side),
        scratch_shapes=[
            pltpu.VMEM((ff, d), bf16),
            pltpu.VMEM((group, d), bf16),
            *[pltpu.VMEM((group, ff), bf16)] * 5,
            *[pltpu.VMEM((2, dt, ff), bf16)] * 2,
            pltpu.VMEM((2, group, dt), bf16),
            pltpu.SemaphoreType.DMA((len(LINKS), 2 * (n - 1))),
            pltpu.SemaphoreType.DMA((len(LINKS), 2 * (n - 1))),
            pltpu.SemaphoreType.DMA,
            pltpu.SemaphoreType.DMA((3, 4)),
            pltpu.SemaphoreType.DMA((3, 4)),
            pltpu.SemaphoreType.DMA((2, 2)),
            pltpu.SemaphoreType.DMA((2, 4)),
        ],
        compiler_params=pltpu.CompilerParams(
            collective_id=0, has_side_effects=True, vmem_limit_bytes=60 * 1024 * 1024
        ),
        cost_estimate=pl.CostEstimate(
            flops=flops, bytes_accessed=2 * (8 * 2 * d * ff + 6 * tokens * d), transcendentals=tokens * ff
        ),
        name="gather_and_dx",
    )(x, dy, gate, up, wg, wu, wd)


def dw_in_kernel(after, *refs):
    x_ref, d_ref = refs[:2]
    dwg_ref, dwu_ref = refs[-2:]
    ff = dwg_ref.shape[1]
    dw = lax.dot_general(
        x_ref[...], d_ref[...], (((0,), (0,)), ((), ())), preferred_element_type=jnp.float32
    )
    dwg_ref[...] = dw[:, :ff].astype(dwg_ref.dtype)
    dwu_ref[...] = dw[:, ff:].astype(dwu_ref.dtype)


def dw_in(full, dgu, first, last, so_far=(), after=()):
    _, tokens, d = full.shape
    ff = dgu.shape[1] // 2
    bd = tile_of(d, 256)
    out = jax.ShapeDtypeStruct((d, ff), full.dtype)
    anywhere = pl.BlockSpec(memory_space=pl.ANY)
    n = last - first
    return pl.pallas_call(
        functools.partial(dw_in_kernel, len(after)),
        grid=(n,),
        out_shape=(out, out),
        in_specs=[
            pl.BlockSpec((pl.squeezed, tokens, bd), lambda i: (1, 0, i + first)),
            pl.BlockSpec((tokens, 2 * ff), lambda i: (0, 0), pipeline_mode=pl.Buffered(1)),
            *[anywhere] * (len(so_far) + len(after)),
        ],
        out_specs=[pl.BlockSpec((bd, ff), lambda i: (i + first, 0))] * 2,
        input_output_aliases={2 + i: i for i in range(len(so_far))},
        compiler_params=pltpu.CompilerParams(vmem_limit_bytes=60 * 1024 * 1024),
        cost_estimate=pl.CostEstimate(
            flops=4 * tokens * n * bd * ff, bytes_accessed=2 * (tokens * n * bd + 2 * ff * (tokens + n * bd)), transcendentals=0
        ),
        name="dw_in",
    )(full, dgu, *so_far, *after)


def dw_out_kernel(h_ref, dy_ref, dw_ref, ht):
    @pl.when(pl.program_id(0) == 0)
    def _():
        ht[...] = h_ref[...].T

    dw = jnp.dot(ht[...], dy_ref[...], preferred_element_type=jnp.float32)
    dw_ref[...] = dw.astype(dw_ref.dtype)


def dw_out(full, hidden):
    _, tokens, d = full.shape
    ff = hidden.shape[1]
    bd = tile_of(d, 512)
    return pl.pallas_call(
        dw_out_kernel,
        grid=(d // bd,),
        out_shape=jax.ShapeDtypeStruct((ff, d), full.dtype),
        in_specs=[
            pl.BlockSpec((tokens, ff), lambda i: (0, 0), pipeline_mode=pl.Buffered(1)),
            pl.BlockSpec((pl.squeezed, tokens, bd), lambda i: (0, 0, i)),
        ],
        out_specs=pl.BlockSpec((ff, bd), lambda i: (0, i)),
        scratch_shapes=[pltpu.VMEM((ff, tokens), full.dtype)],
        compiler_params=pltpu.CompilerParams(vmem_limit_bytes=60 * 1024 * 1024),
        cost_estimate=pl.CostEstimate(
            flops=2 * tokens * d * ff, bytes_accessed=2 * (tokens * d + ff * (tokens + d)), transcendentals=0
        ),
        name="dw_out",
    )(hidden, full)


def f32(v):
    return v.astype(jnp.float32)


def bf16(v):
    return v.astype(jnp.bfloat16)


def exchange(hop, t, one, two):
    far = [hop(t[2][0], one, 1), hop(t[2][1], one, -1)]
    raw = [hop(t[1][1], one, 1), hop(t[3][0], one, -1)]
    near = [bf16(f32(t[1][0]) + f32(far[0])), bf16(f32(t[3][1]) + f32(far[1]))]
    yield near
    near = [hop(near[0], one, 1), hop(near[1], one, -1)]
    plus, minus = [near[0], raw[0]], [raw[1], near[1]]

    def piece(j, r):
        return f32(t[0][r][j]) + f32(plus[r][j]) + f32(minus[r][j])

    far = [bf16(piece(2, 0)), bf16(piece(2, 1))]
    raw = [bf16(piece(1, 1)), bf16(piece(3, 0))]
    yield [*far, *raw]
    far = [hop(far[0], two, 1), hop(far[1], two, -1)]
    raw = [hop(raw[0], two, 1), hop(raw[1], two, -1)]
    near = [bf16(piece(1, 0) + f32(far[0])), bf16(piece(3, 1) + f32(far[1]))]
    yield near
    near = [hop(near[0], two, 1), hop(near[1], two, -1)]
    last_plus, last_minus = [near[0], raw[0]], [raw[1], near[1]]
    yield [(t[0][r], plus[r], minus[r], last_plus[r], last_minus[r]) for r in range(2)]


def total_kernel(chunks, *refs):
    *ins, out_ref = refs
    half = ins[0].shape[0]
    for h in range(2):

        @pl.when(pl.program_id(0) // chunks == h)
        def _():
            for r in range(2):
                parts = ins[10 * h + 5 * r :][:5]
                total = f32(parts[0][...])
                for part in parts[1:]:
                    total += f32(part[...])
                out_ref[r * half : (r + 1) * half, :] = bf16(total)


def total(halves):
    half, cols = halves[0][0][-1].shape
    chunk = tile_of(cols, 896)
    chunks = cols // chunk
    specs, args = [], []
    for h, parts in enumerate(halves):
        col = (lambda i: jnp.minimum(i, chunks - 1)) if h == 0 else (lambda i: jnp.maximum(i - chunks, 0))
        for r in range(2):
            for v in parts[r]:
                args.append(v)
                if v.ndim == 3:
                    specs.append(pl.BlockSpec((pl.squeezed, half, chunk), lambda i, col=col: (0, 0, col(i))))
                else:
                    specs.append(pl.BlockSpec((half, chunk), lambda i, col=col: (0, col(i))))
    return pl.pallas_call(
        functools.partial(total_kernel, chunks),
        grid=(2 * chunks,),
        out_shape=jax.ShapeDtypeStruct((2 * half, 2 * cols), jnp.bfloat16),
        in_specs=specs,
        out_specs=pl.BlockSpec((2 * half, chunk), lambda i: (0, i)),
        cost_estimate=pl.CostEstimate(flops=16 * half * cols, bytes_accessed=48 * half * cols, transcendentals=0),
        compiler_params=pltpu.CompilerParams(vmem_limit_bytes=60 * 1024 * 1024),
        name="dx_total",
    )(*args)


def solution(mesh):
    side = math.isqrt(mesh.shape["tp"])

    def hop(v, axis, sign):
        pairs = []
        for i in range(side * side):
            at = [i // side, i % side]
            at[axis] = (at[axis] + sign) % side
            pairs.append((i, at[0] * side + at[1]))
        return lax.ppermute(v, "tp", pairs)

    def device_step(x, dy, gate, up, w_gate, w_up, w_down):
        full, dgu, hidden, *terms = gather(side, x, dy, gate, up, w_gate, w_up, w_down)
        blocks = x.shape[1] // tile_of(x.shape[1], 256)
        cuts = [0, blocks * 5 // 7, blocks * 6 // 7, blocks]
        halves = [
            exchange(hop, [terms[4 * side // 2 * h + 2 * k :][:2] for k in range(side)], h, 1 - h)
            for h in range(2)
        ]
        dw_down = dw_out(full, hidden)
        near = [next(e) for e in halves]
        dw = dw_in(full, dgu, cuts[0], cuts[1], after=[v for n in near for v in n])
        turn = [next(e) for e in halves]
        dw = dw_in(full, dgu, cuts[1], cuts[2], dw, after=[v for n in turn for v in n])
        near = [next(e) for e in halves]
        dw = dw_in(full, dgu, cuts[2], cuts[3], dw, after=[v for n in near for v in n])
        dx = total([next(e) for e in halves])
        return dx, *dw, dw_down

    rows, both, cols = P(("dp", "tp"), None), P("dp", "tp"), P(None, "tp")
    return jax.shard_map(
        device_step,
        mesh=mesh,
        in_specs=(rows, rows, both, both, cols, cols, P("tp", None)),
        out_specs=(rows, both, both, rows),
        check_vma=False,
    )
```

```python
import functools
import math

import jax
import jax.numpy as jnp
from jax import lax
from jax.experimental import pallas as pl
from jax.experimental.pallas import tpu as pltpu
from jax.sharding import PartitionSpec as P

MESH = pl.DeviceIdType.MESH
LINKS = ((0, 1), (0, -1), (1, 1), (1, -1))
TICKS = 2
FIRST = 6
VMEM = 65400 * 1024
PARTS = 3


def tile_of(size, want):
    return want if size % want == 0 else size


def gather_kernel(
    side, dt, nt,
    x_ref, dy_ref, gate_ref, up_ref, wg_ref, wu_ref, wd_ref,
    full_ref, dgu_ref, hid_ref, dwd_ref, *rest,
):
    terms, scratch = rest[: 4 * side], rest[4 * side :]
    (
    wd_v, dy_v, g_v, u_v, dg_v, du_v, h_v, wg_t, wu_t, out_t, hid_v, ht_v, dy_t, dwd_t,
    send_sem, recv_sem, wd_sem, in_sem, res_sem, w_sem, out_sem, hid_sem, dyt_sem, dwd_sem,
    ) = scratch
    rows, d = dy_ref.shape
    ff = gate_ref.shape[1]
    half, cols = rows // 2, d // 2
    ring = side - 1
    slots = side * side - 1
    me = lax.axis_index("tp")
    at = (me // side, me % side)

    def owner(da, db):
        return lax.rem(at[0] + da + 2 * side, side) * side + lax.rem(at[1] + db + 2 * side, side)

    def on_link(link, along, across):
        axis, sign = link
        steps = (sign * along, sign * across)
        return owner(*(steps if axis == 0 else steps[::-1]))

    def unit(link, slot, back):
        array, s = slot // slots, slot % slots
        early = s < 2 * ring
        late = jnp.maximum(s - 2 * ring, 0)
        hop = jnp.where(early, s // 2, late // ring) + 1
        across = jnp.where(early, 0, late % ring + 1)
        second = jnp.where(early, s % 2, 1)
        who = on_link(link, back - hop, -across)
        axis, sign = link
        col = second if axis == 0 else 1 - second
        row = pl.multiple_of(who * rows + (0 if sign == 1 else half), 8)
        return full_ref.at[array, pl.ds(row, half), pl.ds(pl.multiple_of(col * cols, 128), cols)]

    def copy(k, slot, src, dst):
        return pltpu.make_async_remote_copy(
            src_ref=src,
            dst_ref=dst,
            send_sem=send_sem.at[k, slot],
            recv_sem=recv_sem.at[k, slot],
            device_id={"tp": on_link(LINKS[k], 1, 0)},
            device_id_type=MESH,
        )

    def send(slot):
        for k, link in enumerate(LINKS):
            part = unit(link, slot, 1)
            copy(k, slot, part, part).start()

    def arrive(slot):
        for k, link in enumerate(LINKS):
            part = unit(link, slot, 0)
            copy(k, slot, part, part).wait_recv()

    def step(slot):
        arrive(slot)

        @pl.when(slot + 2 < 2 * slots)
        def _():
            send(slot + 2)

    barrier = pltpu.get_barrier_semaphore()
    for link in LINKS:
        pl.semaphore_signal(barrier, inc=1, device_id={"tp": on_link(link, 1, 0)}, device_id_type=MESH)
    pl.semaphore_wait(barrier, len(LINKS))

    for slot in range(2):
        for k, (axis, sign) in enumerate(LINKS):
            col = slot if axis == 0 else 1 - slot
            r = 0 if sign == 1 else half
            part = (pl.ds(r, half), pl.ds(col * cols, cols))
            row = pl.multiple_of(me * rows + r, 8)
            copy(k, slot, dy_ref.at[part], full_ref.at[0, pl.ds(row, half), part[1]]).start()

    wd_copy = pltpu.make_async_copy(wd_ref, wd_v, wd_sem)
    wd_copy.start()

    mine = pl.ds(pl.multiple_of(me * rows, 8), rows)
    own = [dy_v.at[pl.ds(i * rows, rows)] for i in range(2)]
    loads = [pltpu.make_async_copy(ref, own[i], in_sem.at[0, i]) for i, ref in enumerate((dy_ref, x_ref))]
    stores = [pltpu.make_async_copy(own[i], full_ref.at[i, mine], in_sem.at[1, i]) for i in range(2)]
    for load in loads:
        load.start()
    for load, store in zip(loads, stores):
        load.wait()
        store.start()
    for store in stores:
        store.wait()

    tiles = d // dt
    cut = tiles // 2

    def weights(i, slot):
        part = pl.ds(pl.multiple_of(i * dt, dt), dt)
        return [
            pltpu.make_async_copy(ref.at[part], buf.at[slot], w_sem.at[j, slot])
            for j, (ref, buf) in enumerate(((wg_ref, wg_t), (wu_ref, wu_t)))
        ]

    for c in weights(0, 0):
        c.start()
    lax.fori_loop(0, FIRST, lambda s, _: (step(s), None)[1], None)
    wd_copy.wait()

    def group(q, p):
        offsets = [2 * p, 2 * p + 1]
        starts = []
        for a in offsets:
            starts += [owner(-a, -q) * rows, owner(a, q) * rows + half]
        local = [pl.ds(i * half, half) for i in range(4)]
        there = [pl.ds(pl.multiple_of(s, 8), half) for s in starts]
        first = FIRST + TICKS * (q * (side // 2) + p)

        step(first)
        reads = [
            pltpu.make_async_copy(ref.at[t], buf.at[h], in_sem.at[j, i])
            for j, (ref, buf) in enumerate(((full_ref.at[0], dy_v), (gate_ref, g_v), (up_ref, u_v)))
            for i, (t, h) in enumerate(zip(there, local))
        ]
        for c in reads:
            c.start()
        for c in reads:
            c.wait()

        def hidden_tile(i, _):
            n = pl.ds(pl.multiple_of(i * nt, nt), nt)
            d_hidden = lax.dot_general(
                dy_v[...], wd_v[n, :], (((1,), (1,)), ((), ())), preferred_element_type=jnp.float32
            )
            gate, up = g_v[:, n].astype(jnp.float32), u_v[:, n].astype(jnp.float32)
            s = jax.nn.sigmoid(gate)
            silu = gate * s
            d_silu = d_hidden * up
            dg_v[:, n] = (d_silu * s + d_silu * gate * (s * (1 - s))).astype(dg_v.dtype)
            du_v[:, n] = (d_hidden * silu).astype(du_v.dtype)
            h_v[:, n] = (silu * up).astype(h_v.dtype)

        lax.fori_loop(0, ff // nt, hidden_tile, None)
        results = [
            pltpu.make_async_copy(buf.at[h], ref.at[t, c], res_sem.at[j, i])
            for j, (buf, ref, c) in enumerate((
                (dg_v, dgu_ref, pl.ds(0, ff)), (du_v, dgu_ref, pl.ds(ff, ff)), (h_v, hid_ref, pl.ds(0, ff)),
            ))
            for i, (t, h) in enumerate(zip(there, local))
        ]
        for c in results:
            c.start()

        def stores_of(i, slot, second, b):
            n = pl.ds(pl.multiple_of((i - second * cut) * dt, dt), dt)
            copies = []
            for j, a in enumerate(offsets):
                for r in range(2):
                    da, db = ((-a) % side, (side - b) % side) if r == 0 else (a, b)
                    key, at_ = (2 * side + 2 * db + r, da) if second else (2 * da + r, db)
                    k = 2 * j + r
                    copies.append(pltpu.make_async_copy(
                        out_t.at[slot, local[k]], terms[key].at[at_, :, n], out_sem.at[slot, k]
                    ))
            return copies

        def for_stores(i, slot, second, act):
            if not second:
                for c in stores_of(i, slot, second, q):
                    act(c)
                return
            for b in range(side):

                @pl.when(q == b)
                def _():
                    for c in stores_of(i, slot, second, b):
                        act(c)

        def dx_tile(second):
            begin = cut if second else 0

            def body(i, _):
                slot = i % 2
                for c in weights(i, slot):
                    c.wait()

                @pl.when((i + 1 < tiles) | (q + 1 < side) | (p + 1 < side // 2))
                def _():
                    for c in weights((i + 1) % tiles, (i + 1) % 2):
                        c.start()

                @pl.when(i >= begin + 2)
                def _():
                    for_stores(i - 2, slot, second, lambda c: c.wait())

                nt_dims = (((1,), (1,)), ((), ()))
                term = lax.dot_general(dg_v[...], wg_t[slot], nt_dims, preferred_element_type=jnp.float32)
                term += lax.dot_general(du_v[...], wu_t[slot], nt_dims, preferred_element_type=jnp.float32)
                out_t[slot] = term.astype(out_t.dtype)
                for_stores(i, slot, second, lambda c: c.start())

            end = tiles if second else cut
            lax.fori_loop(begin, end, body, None)
            for i in range(max(begin, end - 2), end):
                for_stores(i, i % 2, second, lambda c: c.wait())

        step(first + 1)
        dx_tile(False)
        dx_tile(True)
        for c in results:
            c.wait()

    def groups(q, _):
        for p in range(side // 2):
            group(q, p)

    lax.fori_loop(0, side, groups, None)
    done = FIRST + TICKS * side * (side // 2)

    fm = ff // 2
    tokens = hid_ref.shape[0]
    tb = tile_of(tokens, 512)
    per = -(-tiles // PARTS)

    def dy_tile(i):
        n = pl.ds(pl.multiple_of(i * dt, dt), dt)
        return pltpu.make_async_copy(full_ref.at[0, :, n], dy_t.at[i % 2], dyt_sem.at[i % 2])

    def dwd_tile(m, i):
        n = pl.ds(pl.multiple_of(i * dt, dt), dt)
        row = pl.ds(pl.multiple_of(m * fm, fm), fm)
        return pltpu.make_async_copy(dwd_t.at[i % 2], dwd_ref.at[row, n], dwd_sem.at[i % 2])

    dy_tile(0).start()

    def down(m, _):
        load = pltpu.make_async_copy(hid_ref.at[:, pl.ds(pl.multiple_of(m * fm, fm), fm)], hid_v, hid_sem)
        load.start()
        load.wait()
        for b in range(tokens // tb):
            ht_v[:, b * tb : (b + 1) * tb] = hid_v[b * tb : (b + 1) * tb, :].T

        def tile(i, _):
            dy_tile(i).wait()

            @pl.when((i + 1 < tiles) | (m == 0))
            def _():
                dy_tile((i + 1) % tiles).start()

            @pl.when((i >= 2) | (m == 1))
            def _():
                dwd_tile(m, i).wait()

            dw = jnp.dot(ht_v[...], dy_t[i % 2], preferred_element_type=jnp.float32)
            dwd_t[i % 2] = dw.astype(dwd_t.dtype)
            dwd_tile(m, i).start()

        def part(k, _):
            step(done + m * PARTS + k)
            lax.fori_loop(k * per, jnp.minimum((k + 1) * per, tiles), tile, None)

        lax.fori_loop(0, PARTS, part, None)

    lax.fori_loop(0, 2, down, None)
    for i in (tiles - 2, tiles - 1):
        dwd_tile(1, i).wait()
    lax.fori_loop(done + 2 * PARTS, 2 * slots, lambda s, _: (step(s), None)[1], None)

    def sent(slot, _):
        for k, link in enumerate(LINKS):
            part = unit(link, slot, 1)
            copy(k, slot, part, part).wait_send()

    lax.fori_loop(0, 2 * slots, sent, None)


def gather(side, x, dy, gate, up, wg, wu, wd):
    rows, d = dy.shape
    tokens, ff = gate.shape
    n = side * side
    group = 2 * rows
    dt, nt = tile_of(d // 2, 512), tile_of(ff, 256)
    bf16 = jnp.bfloat16
    flops = 8 * tokens * d * ff
    anywhere = pl.BlockSpec(memory_space=pltpu.HBM)
    return pl.pallas_call(
        functools.partial(gather_kernel, side, dt, nt),
        out_shape=(
            jax.ShapeDtypeStruct((2, tokens, d), bf16),
            jax.ShapeDtypeStruct((tokens, 2 * ff), bf16),
            jax.ShapeDtypeStruct((tokens, ff), bf16),
            jax.ShapeDtypeStruct((ff, d), bf16),
            *[jax.ShapeDtypeStruct((side, rows // 2, d // 2), bf16)] * (4 * side),
        ),
        in_specs=[anywhere] * 7,
        out_specs=(anywhere,) * (4 + 4 * side),
        scratch_shapes=[
            pltpu.VMEM((ff, d), bf16),
            pltpu.VMEM((group, d), bf16),
            *[pltpu.VMEM((group, ff), bf16)] * 5,
            *[pltpu.VMEM((2, dt, ff), bf16)] * 2,
            pltpu.VMEM((2, group, dt), bf16),
            pltpu.VMEM((tokens, ff // 2), bf16),
            pltpu.VMEM((ff // 2, tokens), bf16),
            pltpu.VMEM((2, tokens, dt), bf16),
            pltpu.VMEM((2, ff // 2, dt), bf16),
            pltpu.SemaphoreType.DMA((len(LINKS), 2 * (n - 1))),
            pltpu.SemaphoreType.DMA((len(LINKS), 2 * (n - 1))),
            pltpu.SemaphoreType.DMA,
            pltpu.SemaphoreType.DMA((3, 4)),
            pltpu.SemaphoreType.DMA((3, 4)),
            pltpu.SemaphoreType.DMA((2, 2)),
            pltpu.SemaphoreType.DMA((2, 4)),
            pltpu.SemaphoreType.DMA,
            pltpu.SemaphoreType.DMA((2,)),
            pltpu.SemaphoreType.DMA((2,)),
        ],
        compiler_params=pltpu.CompilerParams(
            collective_id=0, has_side_effects=True, vmem_limit_bytes=VMEM
        ),
        cost_estimate=pl.CostEstimate(
            flops=flops, bytes_accessed=2 * (8 * 2 * d * ff + 6 * tokens * d), transcendentals=tokens * ff
        ),
        name="gather_and_dx",
    )(x, dy, gate, up, wg, wu, wd)


def dw_in_kernel(sums, moved, *refs):
    x_ref, d_ref, *rest = refs
    outs = rest[len(rest) - 2 - sums - moved :]
    dwg_ref, dwu_ref = outs[:2]
    ff = dwg_ref.shape[1]
    dw = lax.dot_general(
        x_ref[...], d_ref[...], (((0,), (0,)), ((), ())), preferred_element_type=jnp.float32
    )
    dwg_ref[...] = dw[:, :ff].astype(dwg_ref.dtype)
    dwu_ref[...] = dw[:, ff:].astype(dwu_ref.dtype)
    for k in range(sums):
        mine, came = rest[2 * k : 2 * k + 2]
        outs[2 + k][...] = bf16(f32(mine[...]) + f32(came[...]))
    for k in range(moved):
        outs[2 + sums + k][...] = rest[2 * sums + k][...]


def dw_in(full, dgu, first, last, so_far=(), pairs=(), moved=()):
    _, tokens, d = full.shape
    ff = dgu.shape[1] // 2
    bd = tile_of(d, 256)
    n = last - first
    flat = [v for pair in pairs for v in pair]

    def along(v):
        lead = v.shape[:-1]
        return pl.BlockSpec((*lead, v.shape[-1] // n), lambda i: (*[0] * len(lead), i))

    extra = [a for a, _ in pairs] + list(moved)
    new = [jax.ShapeDtypeStruct((d, ff), full.dtype)] * 2 + [jax.ShapeDtypeStruct(v.shape, v.dtype) for v in extra]
    return pl.pallas_call(
        functools.partial(dw_in_kernel, len(pairs), len(moved)),
        grid=(n,),
        out_shape=new,
        in_specs=[
            pl.BlockSpec((pl.squeezed, tokens, bd), lambda i: (1, 0, i + first)),
            pl.BlockSpec((tokens, 2 * ff), lambda i: (0, 0), pipeline_mode=pl.Buffered(1)),
            *[along(v) for v in (*flat, *moved)],
            *[pl.BlockSpec(memory_space=pltpu.HBM)] * len(so_far),
        ],
        out_specs=[*[pl.BlockSpec((bd, ff), lambda i: (i + first, 0))] * 2, *[along(v) for v in extra]],
        input_output_aliases={2 + len(flat) + len(moved) + i: i for i in range(len(so_far))},
        compiler_params=pltpu.CompilerParams(vmem_limit_bytes=VMEM),
        cost_estimate=pl.CostEstimate(
            flops=4 * tokens * n * bd * ff, bytes_accessed=2 * (tokens * n * bd + 2 * ff * (tokens + n * bd)), transcendentals=0
        ),
        name="dw_in",
    )(full, dgu, *flat, *moved, *so_far)


def f32(v):
    return v.astype(jnp.float32)


def bf16(v):
    return v.astype(jnp.bfloat16)


def finish_kernel(side, *refs):
    ins, (out_ref, in_v, send_v, recv_v, out_v, in_sem, send_sem, recv_sem, out_sem) = refs[:12], refs[12:]
    half, cols = out_v.shape[0] // 2, out_v.shape[1] // 2
    me = lax.axis_index("tp")
    at = (me // side, me % side)

    def neighbour(axis, sign):
        to = [at[0], at[1]]
        to[axis] = lax.rem(to[axis] + sign + side, side)
        return {"tp": to[0] * side + to[1]}

    barrier = pltpu.get_barrier_semaphore()
    for axis, sign in LINKS:
        pl.semaphore_signal(barrier, inc=1, device_id=neighbour(axis, sign), device_id_type=MESH)

    order = (((2, 0), (2, 1)), ((1, 1), (3, 0)), ((1, 0), (3, 1)))

    def loads(h, j, r):
        return [
            pltpu.make_async_copy(ins[6 * h + 3 * r + k].at[j], in_v.at[h, j, r, k], in_sem.at[h, j, r, k])
            for k in range(3)
        ]

    pieces = [p for step in order for p in step] + [(0, 0), (0, 1)]
    for j, r in pieces:
        for h in range(2):
            for c in loads(h, j, r):
                c.start()

    def piece(h, j, r):
        for c in loads(h, j, r):
            c.wait()
        return f32(in_v[h, j, r, 0]) + f32(in_v[h, j, r, 1]) + f32(in_v[h, j, r, 2])

    def message(h, step, way):
        return pltpu.make_async_remote_copy(
            src_ref=send_v.at[h, step, way],
            dst_ref=recv_v.at[h, step, way],
            send_sem=send_sem.at[h, step, way],
            recv_sem=recv_sem.at[h, step, way],
            device_id=neighbour(1 - h, 1 - 2 * way),
            device_id_type=MESH,
        )

    ready = False
    for step, steps in enumerate(order):
        for h in range(2):
            for way, (j, r) in enumerate(steps):
                total = piece(h, j, r)
                if step == 2:
                    message(h, 0, way).wait_recv()
                    total += f32(recv_v[h, 0, way])
                send_v[h, step, way] = bf16(total)
                if not ready:
                    pl.semaphore_wait(barrier, len(LINKS))
                    ready = True
                message(h, step, way).start()
    stores = []
    for step in (1, 2):
        for h in range(2):
            for way in range(2):
                message(h, step, way).wait_recv()
    for h in range(2):
        for r in range(2):
            total = piece(h, 0, r)
            total += f32(recv_v[h, 2 if r == 0 else 1, 0]) + f32(recv_v[h, 1 if r == 0 else 2, 1])
            part = (pl.ds(r * half, half), pl.ds(h * cols, cols))
            out_v[part] = bf16(total)
            stores.append(pltpu.make_async_copy(out_v.at[part], out_ref.at[part], out_sem.at[h, r]))
            stores[-1].start()
    for c in stores:
        c.wait()
    for step in range(3):
        for h in range(2):
            for way in range(2):
                message(h, step, way).wait_send()


def finish(side, ins):
    _, half, cols = ins[0].shape
    anywhere = pl.BlockSpec(memory_space=pltpu.HBM)
    dtype = jnp.bfloat16
    return pl.pallas_call(
        functools.partial(finish_kernel, side),
        out_shape=jax.ShapeDtypeStruct((2 * half, 2 * cols), dtype),
        in_specs=[anywhere] * len(ins),
        out_specs=anywhere,
        scratch_shapes=[
            pltpu.VMEM((2, side, 2, 3, half, cols), dtype),
            pltpu.VMEM((2, 3, 2, half, cols), dtype),
            pltpu.VMEM((2, 3, 2, half, cols), dtype),
            pltpu.VMEM((2 * half, 2 * cols), dtype),
            pltpu.SemaphoreType.DMA((2, side, 2, 3)),
            pltpu.SemaphoreType.DMA((2, 3, 2)),
            pltpu.SemaphoreType.DMA((2, 3, 2)),
            pltpu.SemaphoreType.DMA((2, 2)),
        ],
        compiler_params=pltpu.CompilerParams(
            collective_id=1, has_side_effects=True, vmem_limit_bytes=VMEM
        ),
        cost_estimate=pl.CostEstimate(
            flops=64 * half * cols, bytes_accessed=2 * 52 * half * cols, transcendentals=0
        ),
        name="finish_dx",
    )(*ins)


def solution(mesh):
    side = math.isqrt(mesh.shape["tp"])

    def hop(v, axis, sign):
        pairs = []
        for i in range(side * side):
            at = [i // side, i % side]
            at[axis] = (at[axis] + sign) % side
            pairs.append((i, at[0] * side + at[1]))
        return lax.ppermute(v, "tp", pairs)

    def device_step(x, dy, gate, up, w_gate, w_up, w_down):
        full, dgu, _, dw_down, *terms = gather(side, x, dy, gate, up, w_gate, w_up, w_down)
        t = [[terms[2 * (h * side + k) :][:2] for k in range(side)] for h in range(2)]
        blocks = x.shape[1] // tile_of(x.shape[1], 256)
        cuts = [0, blocks * 10 // 28, blocks * 14 // 28, blocks]
        far = [(hop(v[2][0], h, 1), hop(v[2][1], h, -1)) for h, v in enumerate(t)]
        raw = [(hop(v[1][1], h, 1), hop(v[3][0], h, -1)) for h, v in enumerate(t)]
        dw = dw_in(full, dgu, cuts[0], cuts[1])
        pairs = [(v[1][0], f[0]) for v, f in zip(t, far)] + [(v[3][1], f[1]) for v, f in zip(t, far)]
        *dw, a, b, c, d = dw_in(full, dgu, cuts[1], cuts[2], dw, pairs)
        near = [(hop(up_, h, 1), hop(down, h, -1)) for h, (up_, down) in enumerate(((a, c), (b, d)))]
        *dw, dw_down = dw_in(full, dgu, cuts[2], cuts[3], dw, moved=[dw_down])
        ins = []
        for v, r, n in zip(t, raw, near):
            ins += [v[0][0], n[0], r[1], v[0][1], r[0], n[1]]
        dx = finish(side, ins)
        return dx, *dw, dw_down

    rows, both, cols = P(("dp", "tp"), None), P("dp", "tp"), P(None, "tp")
    return jax.shard_map(
        device_step,
        mesh=mesh,
        in_specs=(rows, rows, both, both, cols, cols, P("tp", None)),
        out_specs=(rows, both, both, rows),
        check_vma=False,
    )
```

```python
import functools
import math

import jax
import jax.numpy as jnp
from jax import lax
from jax.experimental import pallas as pl
from jax.experimental.pallas import tpu as pltpu
from jax.sharding import PartitionSpec as P

MESH = pl.DeviceIdType.MESH
LINKS = ((0, 1), (0, -1), (1, 1), (1, -1))
TICKS = 2
FIRST = 7
VMEM = 65400 * 1024
DEPTH = 4
DEEP = 3
PARTS = 3


def tile_of(size, want):
    return want if size % want == 0 else size


def gather_kernel(
    side, dt, nt,
    x_ref, dy_ref, gate_ref, up_ref, wg_ref, wu_ref, wd_ref,
    full_ref, dgu_ref, hid_ref, dwd_ref, *rest,
):
    terms, scratch = rest[: 4 * side], rest[4 * side :]
    (
    wd_v, dy_v, g_v, u_v, dg_v, du_v, h_v, wg_t, wu_t, out_t, hid_v, ht_v, dy_t, dwd_t,
    send_sem, recv_sem, wd_sem, in_sem, res_sem, w_sem, out_sem, hid_sem, dyt_sem, dwd_sem,
    ) = scratch
    rows, d = dy_ref.shape
    ff = gate_ref.shape[1]
    half, cols = rows // 2, d // 2
    ring = side - 1
    slots = side * side - 1
    me = lax.axis_index("tp")
    at = (me // side, me % side)

    def owner(da, db):
        return lax.rem(at[0] + da + 2 * side, side) * side + lax.rem(at[1] + db + 2 * side, side)

    def on_link(link, along, across):
        axis, sign = link
        steps = (sign * along, sign * across)
        return owner(*(steps if axis == 0 else steps[::-1]))

    def unit(link, slot, back):
        array, s = slot // slots, slot % slots
        early = s < 2 * ring
        late = jnp.maximum(s - 2 * ring, 0)
        hop = jnp.where(early, s // 2, late // ring) + 1
        across = jnp.where(early, 0, late % ring + 1)
        second = jnp.where(early, s % 2, 1)
        who = on_link(link, back - hop, -across)
        axis, sign = link
        col = second if axis == 0 else 1 - second
        row = pl.multiple_of(who * rows + (0 if sign == 1 else half), 8)
        return full_ref.at[array, pl.ds(row, half), pl.ds(pl.multiple_of(col * cols, 128), cols)]

    def copy(k, slot, src, dst):
        return pltpu.make_async_remote_copy(
            src_ref=src,
            dst_ref=dst,
            send_sem=send_sem.at[k, slot],
            recv_sem=recv_sem.at[k, slot],
            device_id={"tp": on_link(LINKS[k], 1, 0)},
            device_id_type=MESH,
        )

    def send(slot):
        for k, link in enumerate(LINKS):
            part = unit(link, slot, 1)
            copy(k, slot, part, part).start()

    def arrive(slot):
        for k, link in enumerate(LINKS):
            part = unit(link, slot, 0)
            copy(k, slot, part, part).wait_recv()

    def step(slot):
        arrive(slot)

        @pl.when(slot + 2 < 2 * slots)
        def _():
            send(slot + 2)

    barrier = pltpu.get_barrier_semaphore()
    for link in LINKS:
        pl.semaphore_signal(barrier, inc=1, device_id={"tp": on_link(link, 1, 0)}, device_id_type=MESH)
    pl.semaphore_wait(barrier, len(LINKS))

    for slot in range(2):
        for k, (axis, sign) in enumerate(LINKS):
            col = slot if axis == 0 else 1 - slot
            r = 0 if sign == 1 else half
            part = (pl.ds(r, half), pl.ds(col * cols, cols))
            row = pl.multiple_of(me * rows + r, 8)
            copy(k, slot, dy_ref.at[part], full_ref.at[0, pl.ds(row, half), part[1]]).start()

    wd_copy = pltpu.make_async_copy(wd_ref, wd_v, wd_sem)
    wd_copy.start()

    mine = pl.ds(pl.multiple_of(me * rows, 8), rows)
    own = [dy_v.at[pl.ds(i * rows, rows)] for i in range(2)]
    loads = [pltpu.make_async_copy(ref, own[i], in_sem.at[0, i]) for i, ref in enumerate((dy_ref, x_ref))]
    stores = [pltpu.make_async_copy(own[i], full_ref.at[i, mine], in_sem.at[1, i]) for i in range(2)]
    for load in loads:
        load.start()
    for load, store in zip(loads, stores):
        load.wait()
        store.start()
    for store in stores:
        store.wait()

    tiles = d // dt
    cut = tiles // 2

    count = side * (side // 2) * tiles

    def weights(i, slot):
        part = pl.ds(pl.multiple_of(i * dt, dt), dt)
        return [
            pltpu.make_async_copy(ref.at[part], buf.at[slot], w_sem.at[j, slot])
            for j, (ref, buf) in enumerate(((wg_ref, wg_t), (wu_ref, wu_t)))
        ]

    for i in range(DEPTH - 1):
        for c in weights(i % tiles, i):
            c.start()
    lax.fori_loop(0, FIRST, lambda s, _: (step(s), None)[1], None)
    wd_copy.wait()

    local = [pl.ds(i * half, half) for i in range(4)]

    def rows_of(q, p):
        starts = []
        for a in (2 * p, 2 * p + 1):
            starts += [owner(-a, -q) * rows, owner(a, q) * rows + half]
        return [pl.ds(pl.multiple_of(s, 8), half) for s in starts]

    def reads(q, p):
        return [
            pltpu.make_async_copy(ref.at[t], buf.at[h], in_sem.at[j, i])
            for j, (ref, buf) in enumerate(((full_ref.at[0], dy_v), (gate_ref, g_v), (up_ref, u_v)))
            for i, (t, h) in enumerate(zip(rows_of(q, p), local))
        ]

    def group(q, p):
        offsets = [2 * p, 2 * p + 1]
        there = rows_of(q, p)
        which = q * (side // 2) + p
        first = FIRST + TICKS * which

        step(first)
        for c in reads(q, p):
            c.wait()

        def hidden_tile(i, _):
            n = pl.ds(pl.multiple_of(i * nt, nt), nt)
            d_hidden = lax.dot_general(
                dy_v[...], wd_v[n, :], (((1,), (1,)), ((), ())), preferred_element_type=jnp.float32
            )
            gate, up = g_v[:, n].astype(jnp.float32), u_v[:, n].astype(jnp.float32)
            s = jax.nn.sigmoid(gate)
            silu = gate * s
            d_silu = d_hidden * up
            dg_v[:, n] = (d_silu * s + d_silu * gate * (s * (1 - s))).astype(dg_v.dtype)
            du_v[:, n] = (d_hidden * silu).astype(du_v.dtype)
            h_v[:, n] = (silu * up).astype(h_v.dtype)

        lax.fori_loop(0, ff // nt, hidden_tile, None)
        results = [
            pltpu.make_async_copy(buf.at[h], ref.at[t, c], res_sem.at[j, i])
            for j, (buf, ref, c) in enumerate((
                (dg_v, dgu_ref, pl.ds(0, ff)), (du_v, dgu_ref, pl.ds(ff, ff)), (h_v, hid_ref, pl.ds(0, ff)),
            ))
            for i, (t, h) in enumerate(zip(there, local))
        ]
        for c in results:
            c.start()
        step(first + 1)

        @pl.when(which + 1 < side * (side // 2))
        def _():
            for c in reads(q + (p + 1) // (side // 2), (p + 1) % (side // 2)):
                c.start()

        def stores_of(i, slot, second, b):
            n = pl.ds(pl.multiple_of((i - second * cut) * dt, dt), dt)
            copies = []
            for j, a in enumerate(offsets):
                for r in range(2):
                    da, db = ((-a) % side, (side - b) % side) if r == 0 else (a, b)
                    key, at_ = (2 * side + 2 * db + r, da) if second else (2 * da + r, db)
                    k = 2 * j + r
                    copies.append(pltpu.make_async_copy(
                        out_t.at[slot, local[k]], terms[key].at[at_, :, n], out_sem.at[slot, k]
                    ))
            return copies

        def for_stores(i, slot, second, act):
            if not second:
                for c in stores_of(i, slot, second, q):
                    act(c)
                return
            for b in range(side):

                @pl.when(q == b)
                def _():
                    for c in stores_of(i, slot, second, b):
                        act(c)

        def dx_tile(second):
            begin = cut if second else 0

            def body(i, _):
                at_ = which * tiles + i
                slot = at_ % DEPTH
                for c in weights(i, slot):
                    c.wait()

                @pl.when(at_ + DEPTH - 1 < count)
                def _():
                    for c in weights((i + DEPTH - 1) % tiles, (at_ + DEPTH - 1) % DEPTH):
                        c.start()

                @pl.when(at_ >= DEPTH)
                def _():
                    for c in stores_of(0, slot, False, q):
                        c.wait()

                nt_dims = (((1,), (1,)), ((), ()))
                term = lax.dot_general(dg_v[...], wg_t[slot], nt_dims, preferred_element_type=jnp.float32)
                term += lax.dot_general(du_v[...], wu_t[slot], nt_dims, preferred_element_type=jnp.float32)
                out_t[slot] = term.astype(out_t.dtype)
                for_stores(i, slot, second, lambda c: c.start())

            lax.fori_loop(begin, tiles if second else cut, body, None)

        dx_tile(False)
        dx_tile(True)
        for c in results:
            c.wait()

        if p == side // 2 - 1:

            @pl.when(q == side - 1)
            def _():
                for slot in range(DEPTH):
                    for c in stores_of(0, slot, False, q):
                        c.wait()

    def groups(q, _):
        for p in range(side // 2):
            group(q, p)

    for c in reads(0, 0):
        c.start()
    lax.fori_loop(0, side, groups, None)
    done = FIRST + TICKS * side * (side // 2)

    fm = ff // 2
    tokens = hid_ref.shape[0]
    tb = tile_of(tokens, 512)
    per = -(-tiles // PARTS)

    def dy_tile(i, slot):
        n = pl.ds(pl.multiple_of(i * dt, dt), dt)
        return pltpu.make_async_copy(full_ref.at[0, :, n], dy_t.at[slot], dyt_sem.at[slot])

    def dwd_tile(m, i, slot):
        n = pl.ds(pl.multiple_of(i * dt, dt), dt)
        row = pl.ds(pl.multiple_of(m * fm, fm), fm)
        return pltpu.make_async_copy(dwd_t.at[slot], dwd_ref.at[row, n], dwd_sem.at[slot])

    for i in range(DEEP - 1):
        dy_tile(i % tiles, i).start()

    def down(m, _):
        load = pltpu.make_async_copy(hid_ref.at[:, pl.ds(pl.multiple_of(m * fm, fm), fm)], hid_v, hid_sem)
        load.start()
        load.wait()
        for b in range(tokens // tb):
            ht_v[:, b * tb : (b + 1) * tb] = hid_v[b * tb : (b + 1) * tb, :].T

        def tile(i, _):
            at_ = m * tiles + i
            slot = at_ % DEEP
            dy_tile(i, slot).wait()

            @pl.when(at_ + DEEP - 1 < 2 * tiles)
            def _():
                dy_tile((i + DEEP - 1) % tiles, (at_ + DEEP - 1) % DEEP).start()

            @pl.when(at_ >= DEEP)
            def _():
                dwd_tile(m, i, slot).wait()

            dw = jnp.dot(ht_v[...], dy_t[slot], preferred_element_type=jnp.float32)
            dwd_t[slot] = dw.astype(dwd_t.dtype)
            dwd_tile(m, i, slot).start()

        def part(k, _):
            step(done + m * PARTS + k)
            lax.fori_loop(k * per, jnp.minimum((k + 1) * per, tiles), tile, None)

        lax.fori_loop(0, PARTS, part, None)

    lax.fori_loop(0, 2, down, None)
    for slot in range(DEEP):
        dwd_tile(1, 0, slot).wait()
    lax.fori_loop(done + 2 * PARTS, 2 * slots, lambda s, _: (step(s), None)[1], None)

    def sent(slot, _):
        for k, link in enumerate(LINKS):
            part = unit(link, slot, 1)
            copy(k, slot, part, part).wait_send()

    lax.fori_loop(0, 2 * slots, sent, None)


def gather(side, x, dy, gate, up, wg, wu, wd):
    rows, d = dy.shape
    tokens, ff = gate.shape
    n = side * side
    group = 2 * rows
    dt, nt = tile_of(d // 2, 512), tile_of(ff, 256)
    bf16 = jnp.bfloat16
    flops = 8 * tokens * d * ff
    anywhere = pl.BlockSpec(memory_space=pltpu.HBM)
    return pl.pallas_call(
        functools.partial(gather_kernel, side, dt, nt),
        out_shape=(
            jax.ShapeDtypeStruct((2, tokens, d), bf16),
            jax.ShapeDtypeStruct((tokens, 2 * ff), bf16),
            jax.ShapeDtypeStruct((tokens, ff), bf16),
            jax.ShapeDtypeStruct((ff, d), bf16),
            *[jax.ShapeDtypeStruct((side, rows // 2, d // 2), bf16)] * (4 * side),
        ),
        in_specs=[anywhere] * 7,
        out_specs=(anywhere,) * (4 + 4 * side),
        scratch_shapes=[
            pltpu.VMEM((ff, d), bf16),
            pltpu.VMEM((group, d), bf16),
            *[pltpu.VMEM((group, ff), bf16)] * 5,
            *[pltpu.VMEM((DEPTH, dt, ff), bf16)] * 2,
            pltpu.VMEM((DEPTH, group, dt), bf16),
            pltpu.VMEM((tokens, ff // 2), bf16),
            pltpu.VMEM((ff // 2, tokens), bf16),
            pltpu.VMEM((DEEP, tokens, dt), bf16),
            pltpu.VMEM((DEEP, ff // 2, dt), bf16),
            pltpu.SemaphoreType.DMA((len(LINKS), 2 * (n - 1))),
            pltpu.SemaphoreType.DMA((len(LINKS), 2 * (n - 1))),
            pltpu.SemaphoreType.DMA,
            pltpu.SemaphoreType.DMA((3, 4)),
            pltpu.SemaphoreType.DMA((3, 4)),
            pltpu.SemaphoreType.DMA((2, DEPTH)),
            pltpu.SemaphoreType.DMA((DEPTH, 4)),
            pltpu.SemaphoreType.DMA,
            pltpu.SemaphoreType.DMA((DEEP,)),
            pltpu.SemaphoreType.DMA((DEEP,)),
        ],
        compiler_params=pltpu.CompilerParams(
            collective_id=0, has_side_effects=True, vmem_limit_bytes=VMEM
        ),
        cost_estimate=pl.CostEstimate(
            flops=flops, bytes_accessed=2 * (8 * 2 * d * ff + 6 * tokens * d), transcendentals=tokens * ff
        ),
        name="gather_and_dx",
    )(x, dy, gate, up, wg, wu, wd)


def dw_in_kernel(sums, moved, *refs):
    x_ref, d_ref, *rest = refs
    outs = rest[len(rest) - 2 - sums - moved :]
    dwg_ref, dwu_ref = outs[:2]
    ff = dwg_ref.shape[1]
    dw = lax.dot_general(
        x_ref[...], d_ref[...], (((0,), (0,)), ((), ())), preferred_element_type=jnp.float32
    )
    dwg_ref[...] = dw[:, :ff].astype(dwg_ref.dtype)
    dwu_ref[...] = dw[:, ff:].astype(dwu_ref.dtype)
    for k in range(sums):
        mine, came = rest[2 * k : 2 * k + 2]
        outs[2 + k][...] = bf16(f32(mine[...]) + f32(came[...]))
    for k in range(moved):
        outs[2 + sums + k][...] = rest[2 * sums + k][...]


def dw_in(full, dgu, first, last, so_far=(), pairs=(), moved=()):
    _, tokens, d = full.shape
    ff = dgu.shape[1] // 2
    bd = tile_of(d, 256)
    n = last - first
    flat = [v for pair in pairs for v in pair]

    def along(v):
        lead = v.shape[:-1]
        return pl.BlockSpec((*lead, v.shape[-1] // n), lambda i: (*[0] * len(lead), i))

    extra = [a for a, _ in pairs] + list(moved)
    new = [jax.ShapeDtypeStruct((d, ff), full.dtype)] * 2 + [jax.ShapeDtypeStruct(v.shape, v.dtype) for v in extra]
    return pl.pallas_call(
        functools.partial(dw_in_kernel, len(pairs), len(moved)),
        grid=(n,),
        out_shape=new,
        in_specs=[
            pl.BlockSpec((pl.squeezed, tokens, bd), lambda i: (1, 0, i + first)),
            pl.BlockSpec((tokens, 2 * ff), lambda i: (0, 0), pipeline_mode=pl.Buffered(1)),
            *[along(v) for v in (*flat, *moved)],
            *[pl.BlockSpec(memory_space=pltpu.HBM)] * len(so_far),
        ],
        out_specs=[*[pl.BlockSpec((bd, ff), lambda i: (i + first, 0))] * 2, *[along(v) for v in extra]],
        input_output_aliases={2 + len(flat) + len(moved) + i: i for i in range(len(so_far))},
        compiler_params=pltpu.CompilerParams(vmem_limit_bytes=VMEM),
        cost_estimate=pl.CostEstimate(
            flops=4 * tokens * n * bd * ff, bytes_accessed=2 * (tokens * n * bd + 2 * ff * (tokens + n * bd)), transcendentals=0
        ),
        name="dw_in",
    )(full, dgu, *flat, *moved, *so_far)


def f32(v):
    return v.astype(jnp.float32)


def bf16(v):
    return v.astype(jnp.bfloat16)


def finish_kernel(side, *refs):
    ins, (out_ref, in_v, send_v, recv_v, out_v, in_sem, send_sem, recv_sem, out_sem) = refs[:12], refs[12:]
    half, cols = out_v.shape[0] // 2, out_v.shape[1] // 2
    me = lax.axis_index("tp")
    at = (me // side, me % side)

    def neighbour(axis, sign):
        to = [at[0], at[1]]
        to[axis] = lax.rem(to[axis] + sign + side, side)
        return {"tp": to[0] * side + to[1]}

    barrier = pltpu.get_barrier_semaphore()
    for axis, sign in LINKS:
        pl.semaphore_signal(barrier, inc=1, device_id=neighbour(axis, sign), device_id_type=MESH)

    order = (((2, 0), (2, 1)), ((1, 1), (3, 0)), ((1, 0), (3, 1)))

    def loads(h, j, r):
        return [
            pltpu.make_async_copy(ins[6 * h + 3 * r + k].at[j], in_v.at[h, j, r, k], in_sem.at[h, j, r, k])
            for k in range(3)
        ]

    pieces = [p for step in order for p in step] + [(0, 0), (0, 1)]
    for j, r in pieces:
        for h in range(2):
            for c in loads(h, j, r):
                c.start()

    def piece(h, j, r):
        for c in loads(h, j, r):
            c.wait()
        return f32(in_v[h, j, r, 0]) + f32(in_v[h, j, r, 1]) + f32(in_v[h, j, r, 2])

    def message(h, step, way):
        return pltpu.make_async_remote_copy(
            src_ref=send_v.at[h, step, way],
            dst_ref=recv_v.at[h, step, way],
            send_sem=send_sem.at[h, step, way],
            recv_sem=recv_sem.at[h, step, way],
            device_id=neighbour(1 - h, 1 - 2 * way),
            device_id_type=MESH,
        )

    ready = False
    for step, steps in enumerate(order):
        for h in range(2):
            for way, (j, r) in enumerate(steps):
                total = piece(h, j, r)
                if step == 2:
                    message(h, 0, way).wait_recv()
                    total += f32(recv_v[h, 0, way])
                send_v[h, step, way] = bf16(total)
                if not ready:
                    pl.semaphore_wait(barrier, len(LINKS))
                    ready = True
                message(h, step, way).start()
    stores = []
    for step in (1, 2):
        for h in range(2):
            for way in range(2):
                message(h, step, way).wait_recv()
    for h in range(2):
        for r in range(2):
            total = piece(h, 0, r)
            total += f32(recv_v[h, 2 if r == 0 else 1, 0]) + f32(recv_v[h, 1 if r == 0 else 2, 1])
            part = (pl.ds(r * half, half), pl.ds(h * cols, cols))
            out_v[part] = bf16(total)
            stores.append(pltpu.make_async_copy(out_v.at[part], out_ref.at[part], out_sem.at[h, r]))
            stores[-1].start()
    for c in stores:
        c.wait()
    for step in range(3):
        for h in range(2):
            for way in range(2):
                message(h, step, way).wait_send()


def finish(side, ins):
    _, half, cols = ins[0].shape
    anywhere = pl.BlockSpec(memory_space=pltpu.HBM)
    dtype = jnp.bfloat16
    return pl.pallas_call(
        functools.partial(finish_kernel, side),
        out_shape=jax.ShapeDtypeStruct((2 * half, 2 * cols), dtype),
        in_specs=[anywhere] * len(ins),
        out_specs=anywhere,
        scratch_shapes=[
            pltpu.VMEM((2, side, 2, 3, half, cols), dtype),
            pltpu.VMEM((2, 3, 2, half, cols), dtype),
            pltpu.VMEM((2, 3, 2, half, cols), dtype),
            pltpu.VMEM((2 * half, 2 * cols), dtype),
            pltpu.SemaphoreType.DMA((2, side, 2, 3)),
            pltpu.SemaphoreType.DMA((2, 3, 2)),
            pltpu.SemaphoreType.DMA((2, 3, 2)),
            pltpu.SemaphoreType.DMA((2, 2)),
        ],
        compiler_params=pltpu.CompilerParams(
            collective_id=1, has_side_effects=True, vmem_limit_bytes=VMEM
        ),
        cost_estimate=pl.CostEstimate(
            flops=64 * half * cols, bytes_accessed=2 * 52 * half * cols, transcendentals=0
        ),
        name="finish_dx",
    )(*ins)


def solution(mesh):
    side = math.isqrt(mesh.shape["tp"])

    def hop(v, axis, sign):
        pairs = []
        for i in range(side * side):
            at = [i // side, i % side]
            at[axis] = (at[axis] + sign) % side
            pairs.append((i, at[0] * side + at[1]))
        return lax.ppermute(v, "tp", pairs)

    def device_step(x, dy, gate, up, w_gate, w_up, w_down):
        full, dgu, _, dw_down, *terms = gather(side, x, dy, gate, up, w_gate, w_up, w_down)
        t = [[terms[2 * (h * side + k) :][:2] for k in range(side)] for h in range(2)]
        blocks = x.shape[1] // tile_of(x.shape[1], 256)
        cuts = [0, blocks * 10 // 28, blocks * 14 // 28, blocks]
        far = [(hop(v[2][0], h, 1), hop(v[2][1], h, -1)) for h, v in enumerate(t)]
        raw = [(hop(v[1][1], h, 1), hop(v[3][0], h, -1)) for h, v in enumerate(t)]
        dw = dw_in(full, dgu, cuts[0], cuts[1])
        pairs = [(v[1][0], f[0]) for v, f in zip(t, far)] + [(v[3][1], f[1]) for v, f in zip(t, far)]
        *dw, a, b, c, d = dw_in(full, dgu, cuts[1], cuts[2], dw, pairs)
        near = [(hop(up_, h, 1), hop(down, h, -1)) for h, (up_, down) in enumerate(((a, c), (b, d)))]
        *dw, dw_down = dw_in(full, dgu, cuts[2], cuts[3], dw, moved=[dw_down])
        ins = []
        for v, r, n in zip(t, raw, near):
            ins += [v[0][0], n[0], r[1], v[0][1], r[0], n[1]]
        dx = finish(side, ins)
        return dx, *dw, dw_down

    rows, both, cols = P(("dp", "tp"), None), P("dp", "tp"), P(None, "tp")
    return jax.shard_map(
        device_step,
        mesh=mesh,
        in_specs=(rows, rows, both, both, cols, cols, P("tp", None)),
        out_specs=(rows, both, both, rows),
        check_vma=False,
    )
```

```python
import functools
import math

import jax
import jax.numpy as jnp
from jax import lax
from jax.experimental import pallas as pl
from jax.experimental.pallas import tpu as pltpu
from jax.sharding import PartitionSpec as P

MESH = pl.DeviceIdType.MESH
LINKS = ((0, 1), (0, -1), (1, 1), (1, -1))
TICKS = 2
FIRST = 7
VMEM = 65400 * 1024
DEPTH = 4
DEEP = 3
PARTS = 3


def tile_of(size, want):
    return want if size % want == 0 else size


def gather_kernel(
    side, dt, nt,
    x_ref, dy_ref, gate_ref, up_ref, wg_ref, wu_ref, wd_ref,
    full_ref, dgu_ref, hid_ref, dwd_ref, *rest,
):
    terms, scratch = rest[: 4 * side], rest[4 * side :]
    (
    wd_v, dy_v, g_v, u_v, dg_v, du_v, h_v, wg_t, wu_t, out_t, hid_v, ht_v, dy_t, dwd_t,
    send_sem, recv_sem, wd_sem, in_sem, res_sem, w_sem, out_sem, hid_sem, dyt_sem, dwd_sem,
    ) = scratch
    rows, d = dy_ref.shape
    ff = gate_ref.shape[1]
    half, cols = rows // 2, d // 2
    ring = side - 1
    slots = side * side - 1
    me = lax.axis_index("tp")
    at = (me // side, me % side)

    def owner(da, db):
        return lax.rem(at[0] + da + 2 * side, side) * side + lax.rem(at[1] + db + 2 * side, side)

    def on_link(link, along, across):
        axis, sign = link
        steps = (sign * along, sign * across)
        return owner(*(steps if axis == 0 else steps[::-1]))

    def unit(link, slot, back):
        array, s = slot // slots, slot % slots
        early = s < 2 * ring
        late = jnp.maximum(s - 2 * ring, 0)
        hop = jnp.where(early, s // 2, late // ring) + 1
        across = jnp.where(early, 0, late % ring + 1)
        second = jnp.where(early, s % 2, 1)
        who = on_link(link, back - hop, -across)
        axis, sign = link
        col = second if axis == 0 else 1 - second
        row = pl.multiple_of(who * rows + (0 if sign == 1 else half), 8)
        return full_ref.at[array, pl.ds(row, half), pl.ds(pl.multiple_of(col * cols, 128), cols)]

    def copy(k, slot, src, dst):
        return pltpu.make_async_remote_copy(
            src_ref=src,
            dst_ref=dst,
            send_sem=send_sem.at[k, slot],
            recv_sem=recv_sem.at[k, slot],
            device_id={"tp": on_link(LINKS[k], 1, 0)},
            device_id_type=MESH,
        )

    def send(slot):
        for k, link in enumerate(LINKS):
            part = unit(link, slot, 1)
            copy(k, slot, part, part).start()

    def arrive(slot):
        for k, link in enumerate(LINKS):
            part = unit(link, slot, 0)
            copy(k, slot, part, part).wait_recv()

    def step(slot):
        arrive(slot)

        @pl.when(slot + 2 < 2 * slots)
        def _():
            send(slot + 2)

    barrier = pltpu.get_barrier_semaphore()
    for link in LINKS:
        pl.semaphore_signal(barrier, inc=1, device_id={"tp": on_link(link, 1, 0)}, device_id_type=MESH)
    pl.semaphore_wait(barrier, len(LINKS))

    for slot in range(2):
        for k, (axis, sign) in enumerate(LINKS):
            col = slot if axis == 0 else 1 - slot
            r = 0 if sign == 1 else half
            part = (pl.ds(r, half), pl.ds(col * cols, cols))
            row = pl.multiple_of(me * rows + r, 8)
            copy(k, slot, dy_ref.at[part], full_ref.at[0, pl.ds(row, half), part[1]]).start()

    wd_copy = pltpu.make_async_copy(wd_ref, wd_v, wd_sem)
    wd_copy.start()

    mine = pl.ds(pl.multiple_of(me * rows, 8), rows)
    own = [dy_v.at[pl.ds(i * rows, rows)] for i in range(2)]
    loads = [pltpu.make_async_copy(ref, own[i], in_sem.at[0, i]) for i, ref in enumerate((dy_ref, x_ref))]
    stores = [pltpu.make_async_copy(own[i], full_ref.at[i, mine], in_sem.at[1, i]) for i in range(2)]
    for load in loads:
        load.start()
    for load, store in zip(loads, stores):
        load.wait()
        store.start()
    for store in stores:
        store.wait()

    tiles = d // dt
    cut = tiles // 2

    count = side * (side // 2) * tiles

    def weights(i, slot):
        part = pl.ds(pl.multiple_of(i * dt, dt), dt)
        return [
            pltpu.make_async_copy(ref.at[part], buf.at[slot], w_sem.at[j, slot])
            for j, (ref, buf) in enumerate(((wg_ref, wg_t), (wu_ref, wu_t)))
        ]

    for i in range(DEPTH - 1):
        for c in weights(i % tiles, i):
            c.start()
    lax.fori_loop(0, FIRST, lambda s, _: (step(s), None)[1], None)
    wd_copy.wait()

    local = [pl.ds(i * half, half) for i in range(4)]

    def rows_of(q, p):
        starts = []
        for a in (2 * p, 2 * p + 1):
            starts += [owner(-a, -q) * rows, owner(a, q) * rows + half]
        return [pl.ds(pl.multiple_of(s, 8), half) for s in starts]

    def reads(q, p):
        return [
            pltpu.make_async_copy(ref.at[t], buf.at[h], in_sem.at[j, i])
            for j, (ref, buf) in enumerate(((full_ref.at[0], dy_v), (gate_ref, g_v), (up_ref, u_v)))
            for i, (t, h) in enumerate(zip(rows_of(q, p), local))
        ]

    def group(q, p):
        offsets = [2 * p, 2 * p + 1]
        there = rows_of(q, p)
        which = q * (side // 2) + p
        first = FIRST + TICKS * which

        step(first)
        for c in reads(q, p):
            c.wait()

        def hidden_tile(i, _):
            n = pl.ds(pl.multiple_of(i * nt, nt), nt)
            d_hidden = lax.dot_general(
                dy_v[...], wd_v[n, :], (((1,), (1,)), ((), ())), preferred_element_type=jnp.float32
            )
            gate, up = g_v[:, n].astype(jnp.float32), u_v[:, n].astype(jnp.float32)
            s = jax.nn.sigmoid(gate)
            silu = gate * s
            d_silu = d_hidden * up
            dg_v[:, n] = (d_silu * s + d_silu * gate * (s * (1 - s))).astype(dg_v.dtype)
            du_v[:, n] = (d_hidden * silu).astype(du_v.dtype)
            h_v[:, n] = (silu * up).astype(h_v.dtype)

        lax.fori_loop(0, ff // nt, hidden_tile, None)
        results = [
            pltpu.make_async_copy(buf.at[h], ref.at[t, c], res_sem.at[j, i])
            for j, (buf, ref, c) in enumerate((
                (dg_v, dgu_ref, pl.ds(0, ff)), (du_v, dgu_ref, pl.ds(ff, ff)), (h_v, hid_ref, pl.ds(0, ff)),
            ))
            for i, (t, h) in enumerate(zip(there, local))
        ]
        for c in results:
            c.start()
        step(first + 1)

        @pl.when(which + 1 < side * (side // 2))
        def _():
            for c in reads(q + (p + 1) // (side // 2), (p + 1) % (side // 2)):
                c.start()

        def stores_of(i, slot, second, b):
            n = pl.ds(pl.multiple_of((i - second * cut) * dt, dt), dt)
            copies = []
            for j, a in enumerate(offsets):
                for r in range(2):
                    da, db = ((-a) % side, (side - b) % side) if r == 0 else (a, b)
                    key, at_ = (2 * side + 2 * db + r, da) if second else (2 * da + r, db)
                    k = 2 * j + r
                    copies.append(pltpu.make_async_copy(
                        out_t.at[slot, local[k]], terms[key].at[at_, :, n], out_sem.at[slot, k]
                    ))
            return copies

        def for_stores(i, slot, second, act):
            if not second:
                for c in stores_of(i, slot, second, q):
                    act(c)
                return
            for b in range(side):

                @pl.when(q == b)
                def _():
                    for c in stores_of(i, slot, second, b):
                        act(c)

        def dx_tile(second):
            begin = cut if second else 0

            def body(i, _):
                at_ = which * tiles + i
                slot = at_ % DEPTH
                for c in weights(i, slot):
                    c.wait()

                @pl.when(at_ + DEPTH - 1 < count)
                def _():
                    for c in weights((i + DEPTH - 1) % tiles, (at_ + DEPTH - 1) % DEPTH):
                        c.start()

                @pl.when(at_ >= DEPTH)
                def _():
                    for c in stores_of(0, slot, False, q):
                        c.wait()

                nt_dims = (((1,), (1,)), ((), ()))
                term = lax.dot_general(dg_v[...], wg_t[slot], nt_dims, preferred_element_type=jnp.float32)
                term += lax.dot_general(du_v[...], wu_t[slot], nt_dims, preferred_element_type=jnp.float32)
                out_t[slot] = term.astype(out_t.dtype)
                for_stores(i, slot, second, lambda c: c.start())

            lax.fori_loop(begin, tiles if second else cut, body, None)

        dx_tile(False)
        dx_tile(True)
        for c in results:
            c.wait()

        if p == side // 2 - 1:

            @pl.when(q == side - 1)
            def _():
                for slot in range(DEPTH):
                    for c in stores_of(0, slot, False, q):
                        c.wait()

    def groups(q, _):
        for p in range(side // 2):
            group(q, p)

    for c in reads(0, 0):
        c.start()
    lax.fori_loop(0, side, groups, None)
    done = FIRST + TICKS * side * (side // 2)

    fm = ff // 2
    tokens = hid_ref.shape[0]
    tb = tile_of(tokens, 512)
    per = -(-tiles // PARTS)

    def dy_tile(i, slot):
        n = pl.ds(pl.multiple_of(i * dt, dt), dt)
        return pltpu.make_async_copy(full_ref.at[0, :, n], dy_t.at[slot], dyt_sem.at[slot])

    def dwd_tile(m, i, slot):
        n = pl.ds(pl.multiple_of(i * dt, dt), dt)
        row = pl.ds(pl.multiple_of(m * fm, fm), fm)
        return pltpu.make_async_copy(dwd_t.at[slot], dwd_ref.at[row, n], dwd_sem.at[slot])

    for i in range(DEEP - 1):
        dy_tile(i % tiles, i).start()

    def down(m, _):
        load = pltpu.make_async_copy(hid_ref.at[:, pl.ds(pl.multiple_of(m * fm, fm), fm)], hid_v, hid_sem)
        load.start()
        load.wait()
        for b in range(tokens // tb):
            ht_v[:, b * tb : (b + 1) * tb] = hid_v[b * tb : (b + 1) * tb, :].T

        def tile(i, _):
            at_ = m * tiles + i
            slot = at_ % DEEP
            dy_tile(i, slot).wait()

            @pl.when(at_ + DEEP - 1 < 2 * tiles)
            def _():
                dy_tile((i + DEEP - 1) % tiles, (at_ + DEEP - 1) % DEEP).start()

            @pl.when(at_ >= DEEP)
            def _():
                dwd_tile(m, i, slot).wait()

            dw = jnp.dot(ht_v[...], dy_t[slot], preferred_element_type=jnp.float32)
            dwd_t[slot] = dw.astype(dwd_t.dtype)
            dwd_tile(m, i, slot).start()

        def part(k, _):
            step(done + m * PARTS + k)
            lax.fori_loop(k * per, jnp.minimum((k + 1) * per, tiles), tile, None)

        lax.fori_loop(0, PARTS, part, None)

    lax.fori_loop(0, 2, down, None)
    for slot in range(DEEP):
        dwd_tile(1, 0, slot).wait()
    lax.fori_loop(done + 2 * PARTS, 2 * slots, lambda s, _: (step(s), None)[1], None)

    def sent(slot, _):
        for k, link in enumerate(LINKS):
            part = unit(link, slot, 1)
            copy(k, slot, part, part).wait_send()

    lax.fori_loop(0, 2 * slots, sent, None)


def gather(side, x, dy, gate, up, wg, wu, wd):
    rows, d = dy.shape
    tokens, ff = gate.shape
    n = side * side
    group = 2 * rows
    dt, nt = tile_of(d // 2, 512), tile_of(ff, 256)
    bf16 = jnp.bfloat16
    flops = 8 * tokens * d * ff
    anywhere = pl.BlockSpec(memory_space=pltpu.HBM)
    return pl.pallas_call(
        functools.partial(gather_kernel, side, dt, nt),
        out_shape=(
            jax.ShapeDtypeStruct((2, tokens, d), bf16),
            jax.ShapeDtypeStruct((tokens, 2 * ff), bf16),
            jax.ShapeDtypeStruct((tokens, ff), bf16),
            jax.ShapeDtypeStruct((ff, d), bf16),
            *[jax.ShapeDtypeStruct((side, rows // 2, d // 2), bf16)] * (4 * side),
        ),
        in_specs=[anywhere] * 7,
        out_specs=(anywhere,) * (4 + 4 * side),
        scratch_shapes=[
            pltpu.VMEM((ff, d), bf16),
            pltpu.VMEM((group, d), bf16),
            *[pltpu.VMEM((group, ff), bf16)] * 5,
            *[pltpu.VMEM((DEPTH, dt, ff), bf16)] * 2,
            pltpu.VMEM((DEPTH, group, dt), bf16),
            pltpu.VMEM((tokens, ff // 2), bf16),
            pltpu.VMEM((ff // 2, tokens), bf16),
            pltpu.VMEM((DEEP, tokens, dt), bf16),
            pltpu.VMEM((DEEP, ff // 2, dt), bf16),
            pltpu.SemaphoreType.DMA((len(LINKS), 2 * (n - 1))),
            pltpu.SemaphoreType.DMA((len(LINKS), 2 * (n - 1))),
            pltpu.SemaphoreType.DMA,
            pltpu.SemaphoreType.DMA((3, 4)),
            pltpu.SemaphoreType.DMA((3, 4)),
            pltpu.SemaphoreType.DMA((2, DEPTH)),
            pltpu.SemaphoreType.DMA((DEPTH, 4)),
            pltpu.SemaphoreType.DMA,
            pltpu.SemaphoreType.DMA((DEEP,)),
            pltpu.SemaphoreType.DMA((DEEP,)),
        ],
        compiler_params=pltpu.CompilerParams(
            collective_id=0, has_side_effects=True, vmem_limit_bytes=VMEM
        ),
        cost_estimate=pl.CostEstimate(
            flops=flops, bytes_accessed=2 * (8 * 2 * d * ff + 6 * tokens * d), transcendentals=tokens * ff
        ),
        name="gather_and_dx",
    )(x, dy, gate, up, wg, wu, wd)


def dw_in_kernel(sums, moved, *refs):
    x_ref, d_ref, *rest = refs
    outs = rest[len(rest) - 2 - 2 * sums - moved :]
    dwg_ref, dwu_ref = outs[:2]
    ff = dwg_ref.shape[1]
    dw = lax.dot_general(
        x_ref[...], d_ref[...], (((0,), (0,)), ((), ())), preferred_element_type=jnp.float32
    )
    dwg_ref[...] = dw[:, :ff].astype(dwg_ref.dtype)
    dwu_ref[...] = dw[:, ff:].astype(dwu_ref.dtype)
    for k in range(sums):
        mine, came = rest[2 * k : 2 * k + 2]
        total = bf16(f32(mine[...]) + f32(came[...]))
        outs[2 + 2 * k][...] = total[:1]
        outs[3 + 2 * k][...] = total[1:]
    for k in range(moved):
        outs[2 + 2 * sums + k][...] = rest[2 * sums + k][...]


def dw_in(full, dgu, first, last, so_far=(), pairs=(), moved=()):
    _, tokens, d = full.shape
    ff = dgu.shape[1] // 2
    bd = tile_of(d, 256)
    n = last - first
    flat = [v for pair in pairs for v in pair]

    def along(v):
        lead = v.shape[:-1]
        return pl.BlockSpec((*lead, v.shape[-1] // n), lambda i: (*[0] * len(lead), i))

    cut = [jax.ShapeDtypeStruct((k, *a.shape[1:]), a.dtype) for a, _ in pairs for k in (1, a.shape[0] - 1)]
    extra = [*cut, *moved]
    new = [jax.ShapeDtypeStruct((d, ff), full.dtype)] * 2 + [jax.ShapeDtypeStruct(v.shape, v.dtype) for v in extra]
    return pl.pallas_call(
        functools.partial(dw_in_kernel, len(pairs), len(moved)),
        grid=(n,),
        out_shape=new,
        in_specs=[
            pl.BlockSpec((pl.squeezed, tokens, bd), lambda i: (1, 0, i + first)),
            pl.BlockSpec((tokens, 2 * ff), lambda i: (0, 0), pipeline_mode=pl.Buffered(1)),
            *[along(v) for v in (*flat, *moved)],
            *[pl.BlockSpec(memory_space=pltpu.HBM)] * len(so_far),
        ],
        out_specs=[*[pl.BlockSpec((bd, ff), lambda i: (i + first, 0))] * 2, *[along(v) for v in extra]],
        input_output_aliases={2 + len(flat) + len(moved) + i: i for i in range(len(so_far))},
        compiler_params=pltpu.CompilerParams(vmem_limit_bytes=VMEM),
        cost_estimate=pl.CostEstimate(
            flops=4 * tokens * n * bd * ff, bytes_accessed=2 * (tokens * n * bd + 2 * ff * (tokens + n * bd)), transcendentals=0
        ),
        name="dw_in",
    )(full, dgu, *flat, *moved, *so_far)


def f32(v):
    return v.astype(jnp.float32)


def bf16(v):
    return v.astype(jnp.bfloat16)


def finish_kernel(side, *refs):
    ins, own, rest = refs[:12], refs[12:16], refs[16:]
    out_ref, in_v, send_v, recv_v, own_v, in_sem, send_sem, recv_sem, own_send, own_recv = rest
    half, cols = out_ref.shape[0] // 2, out_ref.shape[1] // 2
    me = lax.axis_index("tp")
    at = (me // side, me % side)

    def neighbour(axis, sign):
        to = [at[0], at[1]]
        to[axis] = lax.rem(to[axis] + sign + side, side)
        return {"tp": to[0] * side + to[1]}

    barrier = pltpu.get_barrier_semaphore()
    for axis, sign in LINKS:
        pl.semaphore_signal(barrier, inc=1, device_id=neighbour(axis, sign), device_id_type=MESH)

    order = (((2, 0), (2, 1)), ((1, 1), (3, 0)), ((1, 0), (3, 1)))

    def loads(h, j, r):
        copies = []
        for k in range(3):
            late = k == 1 + r
            if late and j == 0:
                continue
            src = ins[6 * h + 3 * r + k].at[j - 1 if late else j]
            copies.append(pltpu.make_async_copy(src, in_v.at[h, j, r, k], in_sem.at[h, j, r, k]))
        return copies

    def own_message(h, way):
        return pltpu.make_async_remote_copy(
            src_ref=own[2 * h + way].at[0],
            dst_ref=own_v.at[h, way],
            send_sem=own_send.at[h, way],
            recv_sem=own_recv.at[h, way],
            device_id=neighbour(h, 1 - 2 * way),
            device_id_type=MESH,
        )

    def message(h, step, way):
        return pltpu.make_async_remote_copy(
            src_ref=send_v.at[h, step, way],
            dst_ref=recv_v.at[h, step, way],
            send_sem=send_sem.at[h, step, way],
            recv_sem=recv_sem.at[h, step, way],
            device_id=neighbour(1 - h, 1 - 2 * way),
            device_id_type=MESH,
        )

    def piece(h, j, r):
        for c in loads(h, j, r):
            c.wait()
        total = f32(in_v[h, j, r, 0])
        for k in (1, 2):
            if k == 1 + r and j == 0:
                own_message(h, r).wait_recv()
                total += f32(own_v[h, r])
            else:
                total += f32(in_v[h, j, r, k])
        return total

    pieces = [p for step in order for p in step] + [(0, 0), (0, 1)]
    for j, r in pieces:
        for h in range(2):
            for c in loads(h, j, r):
                c.start()
    pl.semaphore_wait(barrier, len(LINKS))
    for h in range(2):
        for way in range(2):
            own_message(h, way).start()
    for step, steps in enumerate(order):
        for h in range(2):
            for way, (j, r) in enumerate(steps):
                total = piece(h, j, r)
                if step == 2:
                    message(h, 0, way).wait_recv()
                    total += f32(recv_v[h, 0, way])
                send_v[h, step, way] = bf16(total)
                message(h, step, way).start()
    for h in range(2):
        for r in range(2):
            total = piece(h, 0, r)
            message(h, 1, 1 - r).wait_recv()
            total += f32(recv_v[h, 1, 1 - r])
            message(h, 2, r).wait_recv()
            total += f32(recv_v[h, 2, r])
            out_ref[r * half : (r + 1) * half, h * cols : (h + 1) * cols] = bf16(total)
    for h in range(2):
        for way in range(2):
            own_message(h, way).wait_send()
            for step in range(3):
                message(h, step, way).wait_send()


def finish(side, ins, own):
    _, half, cols = ins[0].shape
    hbm = pl.BlockSpec(memory_space=pltpu.HBM)
    dtype = jnp.bfloat16
    return pl.pallas_call(
        functools.partial(finish_kernel, side),
        out_shape=pltpu.VMEM((2 * half, 2 * cols), dtype),
        in_specs=[hbm] * (len(ins) + len(own)),
        out_specs=pl.BlockSpec(memory_space=pltpu.VMEM),
        scratch_shapes=[
            pltpu.VMEM((2, side, 2, 3, half, cols), dtype),
            pltpu.VMEM((2, 3, 2, half, cols), dtype),
            pltpu.VMEM((2, 3, 2, half, cols), dtype),
            pltpu.VMEM((2, 2, half, cols), dtype),
            pltpu.SemaphoreType.DMA((2, side, 2, 3)),
            pltpu.SemaphoreType.DMA((2, 3, 2)),
            pltpu.SemaphoreType.DMA((2, 3, 2)),
            pltpu.SemaphoreType.DMA((2, 2)),
            pltpu.SemaphoreType.DMA((2, 2)),
        ],
        compiler_params=pltpu.CompilerParams(
            collective_id=1, has_side_effects=True, vmem_limit_bytes=54 * 1024 * 1024
        ),
        cost_estimate=pl.CostEstimate(
            flops=64 * half * cols, bytes_accessed=2 * 52 * half * cols, transcendentals=0
        ),
        name="finish_dx",
    )(*ins, *own)


def solution(mesh):
    side = math.isqrt(mesh.shape["tp"])

    def hop(v, axis, sign):
        pairs = []
        for i in range(side * side):
            at = [i // side, i % side]
            at[axis] = (at[axis] + sign) % side
            pairs.append((i, at[0] * side + at[1]))
        return lax.ppermute(v, "tp", pairs)

    def device_step(x, dy, gate, up, w_gate, w_up, w_down):
        full, dgu, _, dw_down, *terms = gather(side, x, dy, gate, up, w_gate, w_up, w_down)
        t = [[terms[2 * (h * side + k) :][:2] for k in range(side)] for h in range(2)]
        blocks = x.shape[1] // tile_of(x.shape[1], 256)
        cuts = [0, blocks * 10 // 28, blocks * 14 // 28, blocks]
        far = [(hop(v[2][0], h, 1), hop(v[2][1], h, -1)) for h, v in enumerate(t)]
        raw = [(hop(v[1][1], h, 1), hop(v[3][0], h, -1)) for h, v in enumerate(t)]
        dw = dw_in(full, dgu, cuts[0], cuts[1])
        pairs = [(v[1][0], f[0]) for v, f in zip(t, far)] + [(v[3][1], f[1]) for v, f in zip(t, far)]
        *dw, a0, a, b0, b, c0, c, d0, d = dw_in(full, dgu, cuts[1], cuts[2], dw, pairs)
        near = [(hop(up_, h, 1), hop(down, h, -1)) for h, (up_, down) in enumerate(((a, c), (b, d)))]
        *dw, dw_down = dw_in(full, dgu, cuts[2], cuts[3], dw, moved=[dw_down])
        ins = []
        for v, r, n in zip(t, raw, near):
            ins += [v[0][0], n[0], r[1], v[0][1], r[0], n[1]]
        dx = finish(side, ins, [a0, c0, b0, d0])
        return dx, *dw, dw_down

    rows, both, cols = P(("dp", "tp"), None), P("dp", "tp"), P(None, "tp")
    return jax.shard_map(
        device_step,
        mesh=mesh,
        in_specs=(rows, rows, both, both, cols, cols, P("tp", None)),
        out_specs=(rows, both, both, rows),
        check_vma=False,
    )
```

```python
import functools
import math

import jax
import jax.numpy as jnp
from jax import lax
from jax.experimental import pallas as pl
from jax.experimental.pallas import tpu as pltpu
from jax.sharding import PartitionSpec as P

MESH = pl.DeviceIdType.MESH
LINKS = ((0, 1), (0, -1), (1, 1), (1, -1))
TICKS = 2
FIRST = 7
VMEM = 65400 * 1024
DEPTH = 4
DEEP = 3
PARTS = 3


def tile_of(size, want):
    return want if size % want == 0 else size


def gather_kernel(
    side, dt, nt,
    x_ref, dy_ref, gate_ref, up_ref, wg_ref, wu_ref, wd_ref,
    full_ref, dgu_ref, hid_ref, dwd_ref, *rest,
):
    terms, scratch = rest[: 4 * side], rest[4 * side :]
    (
    wd_v, dy_v, g_v, u_v, dg_v, du_v, h_v, wg_t, wu_t, out_t, hid_v, ht_v, dy_t, dwd_t,
    send_sem, recv_sem, wd_sem, in_sem, res_sem, w_sem, out_sem, hid_sem, dyt_sem, dwd_sem,
    ) = scratch
    rows, d = dy_ref.shape
    ff = gate_ref.shape[1]
    half, cols = rows // 2, d // 2
    ring = side - 1
    slots = side * side - 1
    me = lax.axis_index("tp")
    at = (me // side, me % side)

    def owner(da, db):
        return lax.rem(at[0] + da + 2 * side, side) * side + lax.rem(at[1] + db + 2 * side, side)

    def on_link(link, along, across):
        axis, sign = link
        steps = (sign * along, sign * across)
        return owner(*(steps if axis == 0 else steps[::-1]))

    def unit(link, slot, back):
        array, s = slot // slots, slot % slots
        early = s < 2 * ring
        late = jnp.maximum(s - 2 * ring, 0)
        hop = jnp.where(early, s // 2, late // ring) + 1
        across = jnp.where(early, 0, late % ring + 1)
        second = jnp.where(early, s % 2, 1)
        who = on_link(link, back - hop, -across)
        axis, sign = link
        col = second if axis == 0 else 1 - second
        row = pl.multiple_of(who * rows + (0 if sign == 1 else half), 8)
        return full_ref.at[array, pl.ds(row, half), pl.ds(pl.multiple_of(col * cols, 128), cols)]

    def copy(k, slot, src, dst):
        return pltpu.make_async_remote_copy(
            src_ref=src,
            dst_ref=dst,
            send_sem=send_sem.at[k, slot],
            recv_sem=recv_sem.at[k, slot],
            device_id={"tp": on_link(LINKS[k], 1, 0)},
            device_id_type=MESH,
        )

    def send(slot):
        for k, link in enumerate(LINKS):
            part = unit(link, slot, 1)
            copy(k, slot, part, part).start()

    def arrive(slot):
        for k, link in enumerate(LINKS):
            part = unit(link, slot, 0)
            copy(k, slot, part, part).wait_recv()

    def step(slot):
        arrive(slot)

        @pl.when(slot + 2 < 2 * slots)
        def _():
            send(slot + 2)

    barrier = pltpu.get_barrier_semaphore()
    for link in LINKS:
        pl.semaphore_signal(barrier, inc=1, device_id={"tp": on_link(link, 1, 0)}, device_id_type=MESH)
    pl.semaphore_wait(barrier, len(LINKS))

    for slot in range(2):
        for k, (axis, sign) in enumerate(LINKS):
            col = slot if axis == 0 else 1 - slot
            r = 0 if sign == 1 else half
            part = (pl.ds(r, half), pl.ds(col * cols, cols))
            row = pl.multiple_of(me * rows + r, 8)
            copy(k, slot, dy_ref.at[part], full_ref.at[0, pl.ds(row, half), part[1]]).start()

    wd_copy = pltpu.make_async_copy(wd_ref, wd_v, wd_sem)
    wd_copy.start()

    mine = pl.ds(pl.multiple_of(me * rows, 8), rows)
    own = [dy_v.at[pl.ds(i * rows, rows)] for i in range(2)]
    loads = [pltpu.make_async_copy(ref, own[i], in_sem.at[0, i]) for i, ref in enumerate((dy_ref, x_ref))]
    stores = [pltpu.make_async_copy(own[i], full_ref.at[i, mine], in_sem.at[1, i]) for i in range(2)]
    for load in loads:
        load.start()
    for load, store in zip(loads, stores):
        load.wait()
        store.start()
    for store in stores:
        store.wait()

    tiles = d // dt
    cut = tiles // 2

    count = side * (side // 2) * tiles

    def weights(i, slot):
        part = pl.ds(pl.multiple_of(i * dt, dt), dt)
        return [
            pltpu.make_async_copy(ref.at[part], buf.at[slot], w_sem.at[j, slot])
            for j, (ref, buf) in enumerate(((wg_ref, wg_t), (wu_ref, wu_t)))
        ]

    for i in range(DEPTH - 1):
        for c in weights(i % tiles, i):
            c.start()
    lax.fori_loop(0, FIRST, lambda s, _: (step(s), None)[1], None)
    wd_copy.wait()

    local = [pl.ds(i * half, half) for i in range(4)]

    def rows_of(q, p):
        starts = []
        for a in (2 * p, 2 * p + 1):
            starts += [owner(-a, -q) * rows, owner(a, q) * rows + half]
        return [pl.ds(pl.multiple_of(s, 8), half) for s in starts]

    def reads(q, p):
        return [
            pltpu.make_async_copy(ref.at[t], buf.at[h], in_sem.at[j, i])
            for j, (ref, buf) in enumerate(((full_ref.at[0], dy_v), (gate_ref, g_v), (up_ref, u_v)))
            for i, (t, h) in enumerate(zip(rows_of(q, p), local))
        ]

    def group(q, p):
        offsets = [2 * p, 2 * p + 1]
        there = rows_of(q, p)
        which = q * (side // 2) + p
        first = FIRST + TICKS * which

        step(first)
        for c in reads(q, p):
            c.wait()

        def hidden_tile(i, _):
            n = pl.ds(pl.multiple_of(i * nt, nt), nt)
            d_hidden = lax.dot_general(
                dy_v[...], wd_v[n, :], (((1,), (1,)), ((), ())), preferred_element_type=jnp.float32
            )
            gate, up = g_v[:, n].astype(jnp.float32), u_v[:, n].astype(jnp.float32)
            s = jax.nn.sigmoid(gate)
            silu = gate * s
            d_silu = d_hidden * up
            dg_v[:, n] = (d_silu * s + d_silu * gate * (s * (1 - s))).astype(dg_v.dtype)
            du_v[:, n] = (d_hidden * silu).astype(du_v.dtype)
            h_v[:, n] = (silu * up).astype(h_v.dtype)

        lax.fori_loop(0, ff // nt, hidden_tile, None)
        results = [
            pltpu.make_async_copy(buf.at[h], ref.at[t, c], res_sem.at[j, i])
            for j, (buf, ref, c) in enumerate((
                (dg_v, dgu_ref, pl.ds(0, ff)), (du_v, dgu_ref, pl.ds(ff, ff)), (h_v, hid_ref, pl.ds(0, ff)),
            ))
            for i, (t, h) in enumerate(zip(there, local))
        ]
        for c in results:
            c.start()
        step(first + 1)

        @pl.when(which + 1 < side * (side // 2))
        def _():
            for c in reads(q + (p + 1) // (side // 2), (p + 1) % (side // 2)):
                c.start()

        def stores_of(i, slot, second, b):
            n = pl.ds(pl.multiple_of((i - second * cut) * dt, dt), dt)
            copies = []
            for j, a in enumerate(offsets):
                for r in range(2):
                    da, db = ((-a) % side, (side - b) % side) if r == 0 else (a, b)
                    key, at_ = (2 * side + 2 * db + r, da) if second else (2 * da + r, db)
                    k = 2 * j + r
                    copies.append(pltpu.make_async_copy(
                        out_t.at[slot, local[k]], terms[key].at[at_, :, n], out_sem.at[slot, k]
                    ))
            return copies

        def for_stores(i, slot, second, act):
            if not second:
                for c in stores_of(i, slot, second, q):
                    act(c)
                return
            for b in range(side):

                @pl.when(q == b)
                def _():
                    for c in stores_of(i, slot, second, b):
                        act(c)

        def dx_tile(second):
            begin = cut if second else 0

            def body(i, _):
                at_ = which * tiles + i
                slot = at_ % DEPTH
                for c in weights(i, slot):
                    c.wait()

                @pl.when(at_ + DEPTH - 1 < count)
                def _():
                    for c in weights((i + DEPTH - 1) % tiles, (at_ + DEPTH - 1) % DEPTH):
                        c.start()

                @pl.when(at_ >= DEPTH)
                def _():
                    for c in stores_of(0, slot, False, q):
                        c.wait()

                nt_dims = (((1,), (1,)), ((), ()))
                term = lax.dot_general(dg_v[...], wg_t[slot], nt_dims, preferred_element_type=jnp.float32)
                term += lax.dot_general(du_v[...], wu_t[slot], nt_dims, preferred_element_type=jnp.float32)
                out_t[slot] = term.astype(out_t.dtype)
                for_stores(i, slot, second, lambda c: c.start())

            lax.fori_loop(begin, tiles if second else cut, body, None)

        dx_tile(False)
        dx_tile(True)
        for c in results:
            c.wait()

        if p == side // 2 - 1:

            @pl.when(q == side - 1)
            def _():
                for slot in range(DEPTH):
                    for c in stores_of(0, slot, False, q):
                        c.wait()

    def groups(q, _):
        for p in range(side // 2):
            group(q, p)

    for c in reads(0, 0):
        c.start()
    lax.fori_loop(0, side, groups, None)
    done = FIRST + TICKS * side * (side // 2)

    fm = ff // 2
    tokens = hid_ref.shape[0]
    tb = tile_of(tokens, 512)
    per = -(-tiles // PARTS)

    def dy_tile(i, slot):
        n = pl.ds(pl.multiple_of(i * dt, dt), dt)
        return pltpu.make_async_copy(full_ref.at[0, :, n], dy_t.at[slot], dyt_sem.at[slot])

    def dwd_tile(m, i, slot):
        n = pl.ds(pl.multiple_of(i * dt, dt), dt)
        row = pl.ds(pl.multiple_of(m * fm, fm), fm)
        return pltpu.make_async_copy(dwd_t.at[slot], dwd_ref.at[row, n], dwd_sem.at[slot])

    for i in range(DEEP - 1):
        dy_tile(i % tiles, i).start()

    def down(m, _):
        load = pltpu.make_async_copy(hid_ref.at[:, pl.ds(pl.multiple_of(m * fm, fm), fm)], hid_v, hid_sem)
        load.start()
        load.wait()
        for b in range(tokens // tb):
            ht_v[:, b * tb : (b + 1) * tb] = hid_v[b * tb : (b + 1) * tb, :].T

        def tile(i, _):
            at_ = m * tiles + i
            slot = at_ % DEEP
            dy_tile(i, slot).wait()

            @pl.when(at_ + DEEP - 1 < 2 * tiles)
            def _():
                dy_tile((i + DEEP - 1) % tiles, (at_ + DEEP - 1) % DEEP).start()

            @pl.when(at_ >= DEEP)
            def _():
                dwd_tile(m, i, slot).wait()

            dw = jnp.dot(ht_v[...], dy_t[slot], preferred_element_type=jnp.float32)
            dwd_t[slot] = dw.astype(dwd_t.dtype)
            dwd_tile(m, i, slot).start()

        def part(k, _):
            step(done + m * PARTS + k)
            lax.fori_loop(k * per, jnp.minimum((k + 1) * per, tiles), tile, None)

        lax.fori_loop(0, PARTS, part, None)

    lax.fori_loop(0, 2, down, None)
    for slot in range(DEEP):
        dwd_tile(1, 0, slot).wait()
    lax.fori_loop(done + 2 * PARTS, 2 * slots, lambda s, _: (step(s), None)[1], None)

    def sent(slot, _):
        for k, link in enumerate(LINKS):
            part = unit(link, slot, 1)
            copy(k, slot, part, part).wait_send()

    lax.fori_loop(0, 2 * slots, sent, None)


def gather(side, x, dy, gate, up, wg, wu, wd):
    rows, d = dy.shape
    tokens, ff = gate.shape
    n = side * side
    group = 2 * rows
    dt, nt = tile_of(d // 2, 512), tile_of(ff, 256)
    bf16 = jnp.bfloat16
    flops = 8 * tokens * d * ff
    anywhere = pl.BlockSpec(memory_space=pltpu.HBM)
    return pl.pallas_call(
        functools.partial(gather_kernel, side, dt, nt),
        out_shape=(
            jax.ShapeDtypeStruct((2, tokens, d), bf16),
            jax.ShapeDtypeStruct((tokens, 2 * ff), bf16),
            jax.ShapeDtypeStruct((tokens, ff), bf16),
            jax.ShapeDtypeStruct((ff, d), bf16),
            *[jax.ShapeDtypeStruct((side, rows // 2, d // 2), bf16)] * (4 * side),
        ),
        in_specs=[anywhere] * 7,
        out_specs=(anywhere,) * (4 + 4 * side),
        scratch_shapes=[
            pltpu.VMEM((ff, d), bf16),
            pltpu.VMEM((group, d), bf16),
            *[pltpu.VMEM((group, ff), bf16)] * 5,
            *[pltpu.VMEM((DEPTH, dt, ff), bf16)] * 2,
            pltpu.VMEM((DEPTH, group, dt), bf16),
            pltpu.VMEM((tokens, ff // 2), bf16),
            pltpu.VMEM((ff // 2, tokens), bf16),
            pltpu.VMEM((DEEP, tokens, dt), bf16),
            pltpu.VMEM((DEEP, ff // 2, dt), bf16),
            pltpu.SemaphoreType.DMA((len(LINKS), 2 * (n - 1))),
            pltpu.SemaphoreType.DMA((len(LINKS), 2 * (n - 1))),
            pltpu.SemaphoreType.DMA,
            pltpu.SemaphoreType.DMA((3, 4)),
            pltpu.SemaphoreType.DMA((3, 4)),
            pltpu.SemaphoreType.DMA((2, DEPTH)),
            pltpu.SemaphoreType.DMA((DEPTH, 4)),
            pltpu.SemaphoreType.DMA,
            pltpu.SemaphoreType.DMA((DEEP,)),
            pltpu.SemaphoreType.DMA((DEEP,)),
        ],
        compiler_params=pltpu.CompilerParams(
            collective_id=0, has_side_effects=True, vmem_limit_bytes=VMEM
        ),
        cost_estimate=pl.CostEstimate(
            flops=flops, bytes_accessed=2 * (8 * 2 * d * ff + 6 * tokens * d), transcendentals=tokens * ff
        ),
        name="gather_and_dx",
    )(x, dy, gate, up, wg, wu, wd)


def dw_in_kernel(sums, moved, *refs):
    x_ref, d_ref, *rest = refs
    outs = rest[len(rest) - 2 - 2 * sums - moved :]
    dwg_ref, dwu_ref = outs[:2]
    ff = dwg_ref.shape[1]
    dw = lax.dot_general(
        x_ref[...], d_ref[...], (((0,), (0,)), ((), ())), preferred_element_type=jnp.float32
    )
    dwg_ref[...] = dw[:, :ff].astype(dwg_ref.dtype)
    dwu_ref[...] = dw[:, ff:].astype(dwu_ref.dtype)
    for k in range(sums):
        mine, came = rest[2 * k : 2 * k + 2]
        total = bf16(f32(mine[...]) + f32(came[...]))
        outs[2 + 2 * k][...] = total[:1]
        outs[3 + 2 * k][...] = total[1:]
    for k in range(moved):
        outs[2 + 2 * sums + k][...] = rest[2 * sums + k][...]


def dw_in(full, dgu, first, last, so_far=(), pairs=(), moved=()):
    _, tokens, d = full.shape
    ff = dgu.shape[1] // 2
    bd = tile_of(d, 256)
    n = last - first
    flat = [v for pair in pairs for v in pair]
    resident = 2 * dgu.size

    def along(v):
        lead = v.shape[:-1]
        return pl.BlockSpec((*lead, v.shape[-1] // n), lambda i: (*[0] * len(lead), i))

    cut = [jax.ShapeDtypeStruct((k, *a.shape[1:]), a.dtype) for a, _ in pairs for k in (1, a.shape[0] - 1)]
    extra = [*cut, *moved]
    new = [jax.ShapeDtypeStruct((d, ff), full.dtype)] * 2 + [jax.ShapeDtypeStruct(v.shape, v.dtype) for v in extra]
    return pl.pallas_call(
        functools.partial(dw_in_kernel, len(pairs), len(moved)),
        grid=(n,),
        out_shape=new,
        in_specs=[
            pl.BlockSpec((pl.squeezed, tokens, bd), lambda i: (1, 0, i + first)),
            pl.BlockSpec(memory_space=pltpu.VMEM),
            *[along(v) for v in (*flat, *moved)],
            *[pl.BlockSpec(memory_space=pltpu.HBM)] * len(so_far),
        ],
        out_specs=[*[pl.BlockSpec((bd, ff), lambda i: (i + first, 0))] * 2, *[along(v) for v in extra]],
        input_output_aliases={2 + len(flat) + len(moved) + i: i for i in range(len(so_far))},
        compiler_params=pltpu.CompilerParams(vmem_limit_bytes=VMEM - resident - 65536),
        cost_estimate=pl.CostEstimate(
            flops=4 * tokens * n * bd * ff, bytes_accessed=2 * (tokens * n * bd + 2 * ff * (tokens + n * bd)), transcendentals=0
        ),
        name="dw_in",
    )(full, dgu, *flat, *moved, *so_far)


def f32(v):
    return v.astype(jnp.float32)


def bf16(v):
    return v.astype(jnp.bfloat16)


def finish_kernel(side, *refs):
    ins, own, rest = refs[:12], refs[12:16], refs[16:]
    out_ref, in_v, send_v, recv_v, own_v, in_sem, send_sem, recv_sem, own_send, own_recv = rest
    half, cols = out_ref.shape[0] // 2, out_ref.shape[1] // 2
    me = lax.axis_index("tp")
    at = (me // side, me % side)

    def neighbour(axis, sign):
        to = [at[0], at[1]]
        to[axis] = lax.rem(to[axis] + sign + side, side)
        return {"tp": to[0] * side + to[1]}

    barrier = pltpu.get_barrier_semaphore()
    for axis, sign in LINKS:
        pl.semaphore_signal(barrier, inc=1, device_id=neighbour(axis, sign), device_id_type=MESH)

    order = (((2, 0), (2, 1)), ((1, 1), (3, 0)), ((1, 0), (3, 1)))

    def loads(h, j, r):
        copies = []
        for k in range(3):
            late = k == 1 + r
            if late and j == 0:
                continue
            src = ins[6 * h + 3 * r + k].at[j - 1 if late else j]
            copies.append(pltpu.make_async_copy(src, in_v.at[h, j, r, k], in_sem.at[h, j, r, k]))
        return copies

    def own_message(h, way):
        return pltpu.make_async_remote_copy(
            src_ref=own[2 * h + way].at[0],
            dst_ref=own_v.at[h, way],
            send_sem=own_send.at[h, way],
            recv_sem=own_recv.at[h, way],
            device_id=neighbour(h, 1 - 2 * way),
            device_id_type=MESH,
        )

    def message(h, step, way):
        return pltpu.make_async_remote_copy(
            src_ref=send_v.at[h, step, way],
            dst_ref=recv_v.at[h, step, way],
            send_sem=send_sem.at[h, step, way],
            recv_sem=recv_sem.at[h, step, way],
            device_id=neighbour(1 - h, 1 - 2 * way),
            device_id_type=MESH,
        )

    def piece(h, j, r):
        for c in loads(h, j, r):
            c.wait()
        total = f32(in_v[h, j, r, 0])
        for k in (1, 2):
            if k == 1 + r and j == 0:
                own_message(h, r).wait_recv()
                total += f32(own_v[h, r])
            else:
                total += f32(in_v[h, j, r, k])
        return total

    pieces = [p for step in order for p in step] + [(0, 0), (0, 1)]
    for j, r in pieces:
        for h in range(2):
            for c in loads(h, j, r):
                c.start()
    pl.semaphore_wait(barrier, len(LINKS))
    for h in range(2):
        for way in range(2):
            own_message(h, way).start()
    for step, steps in enumerate(order):
        for h in range(2):
            for way, (j, r) in enumerate(steps):
                total = piece(h, j, r)
                if step == 2:
                    message(h, 0, way).wait_recv()
                    total += f32(recv_v[h, 0, way])
                send_v[h, step, way] = bf16(total)
                message(h, step, way).start()
    for h in range(2):
        for r in range(2):
            total = piece(h, 0, r)
            message(h, 1, 1 - r).wait_recv()
            total += f32(recv_v[h, 1, 1 - r])
            message(h, 2, r).wait_recv()
            total += f32(recv_v[h, 2, r])
            out_ref[r * half : (r + 1) * half, h * cols : (h + 1) * cols] = bf16(total)
    for h in range(2):
        for way in range(2):
            own_message(h, way).wait_send()
            for step in range(3):
                message(h, step, way).wait_send()


def finish(side, ins, own):
    _, half, cols = ins[0].shape
    hbm = pl.BlockSpec(memory_space=pltpu.HBM)
    dtype = jnp.bfloat16
    return pl.pallas_call(
        functools.partial(finish_kernel, side),
        out_shape=pltpu.VMEM((2 * half, 2 * cols), dtype),
        in_specs=[hbm] * (len(ins) + len(own)),
        out_specs=pl.BlockSpec(memory_space=pltpu.VMEM),
        scratch_shapes=[
            pltpu.VMEM((2, side, 2, 3, half, cols), dtype),
            pltpu.VMEM((2, 3, 2, half, cols), dtype),
            pltpu.VMEM((2, 3, 2, half, cols), dtype),
            pltpu.VMEM((2, 2, half, cols), dtype),
            pltpu.SemaphoreType.DMA((2, side, 2, 3)),
            pltpu.SemaphoreType.DMA((2, 3, 2)),
            pltpu.SemaphoreType.DMA((2, 3, 2)),
            pltpu.SemaphoreType.DMA((2, 2)),
            pltpu.SemaphoreType.DMA((2, 2)),
        ],
        compiler_params=pltpu.CompilerParams(
            collective_id=1, has_side_effects=True, vmem_limit_bytes=54 * 1024 * 1024
        ),
        cost_estimate=pl.CostEstimate(
            flops=64 * half * cols, bytes_accessed=2 * 52 * half * cols, transcendentals=0
        ),
        name="finish_dx",
    )(*ins, *own)


def solution(mesh):
    side = math.isqrt(mesh.shape["tp"])

    def hop(v, axis, sign):
        pairs = []
        for i in range(side * side):
            at = [i // side, i % side]
            at[axis] = (at[axis] + sign) % side
            pairs.append((i, at[0] * side + at[1]))
        return lax.ppermute(v, "tp", pairs)

    def device_step(x, dy, gate, up, w_gate, w_up, w_down):
        full, dgu, _, dw_down, *terms = gather(side, x, dy, gate, up, w_gate, w_up, w_down)
        t = [[terms[2 * (h * side + k) :][:2] for k in range(side)] for h in range(2)]
        dgu = pltpu.with_memory_space_constraint(dgu, pltpu.VMEM)
        blocks = x.shape[1] // tile_of(x.shape[1], 256)
        cuts = [0, blocks * 14 // 28, blocks * 18 // 28, blocks]
        far = [(hop(v[2][0], h, 1), hop(v[2][1], h, -1)) for h, v in enumerate(t)]
        raw = [(hop(v[1][1], h, 1), hop(v[3][0], h, -1)) for h, v in enumerate(t)]
        *dw, dw_down = dw_in(full, dgu, cuts[0], cuts[1], moved=[dw_down])
        pairs = [(v[1][0], f[0]) for v, f in zip(t, far)] + [(v[3][1], f[1]) for v, f in zip(t, far)]
        *dw, a0, a, b0, b, c0, c, d0, d = dw_in(full, dgu, cuts[1], cuts[2], dw, pairs)
        near = [(hop(up_, h, 1), hop(down, h, -1)) for h, (up_, down) in enumerate(((a, c), (b, d)))]
        dw = dw_in(full, dgu, cuts[2], cuts[3], dw)
        ins = []
        for v, r, n in zip(t, raw, near):
            ins += [v[0][0], n[0], r[1], v[0][1], r[0], n[1]]
        dx = finish(side, ins, [a0, c0, b0, d0])
        return dx, *dw, dw_down

    rows, both, cols = P(("dp", "tp"), None), P("dp", "tp"), P(None, "tp")
    return jax.shard_map(
        device_step,
        mesh=mesh,
        in_specs=(rows, rows, both, both, cols, cols, P("tp", None)),
        out_specs=(rows, both, both, rows),
        check_vma=False,
    )
```

```python
import functools
import math

import jax
import jax.numpy as jnp
from jax import lax
from jax.experimental import pallas as pl
from jax.experimental.pallas import tpu as pltpu
from jax.sharding import PartitionSpec as P

MESH = pl.DeviceIdType.MESH
LINKS = ((0, 1), (0, -1), (1, 1), (1, -1))
TICKS = 2
FIRST = 7
VMEM = 65400 * 1024
FINISH = 54 * 1024 * 1024
DEPTH = 4
DEEP = 3
PARTS = 3


def tile_of(size, want):
    return want if size % want == 0 else size


def gather_kernel(
    side, dt, nt,
    x_ref, dy_ref, gate_ref, up_ref, wg_ref, wu_ref, wd_ref,
    full_ref, dgu_ref, hid_ref, dwd_ref, *rest,
):
    terms, scratch = rest[: 4 * side], rest[4 * side :]
    (
    wd_v, dy_v, g_v, u_v, dg_v, du_v, h_v, wg_t, wu_t, out_t, hid_v, ht_v, dy_t, dwd_t,
    send_sem, recv_sem, wd_sem, in_sem, res_sem, w_sem, out_sem, hid_sem, dyt_sem, dwd_sem,
    ) = scratch
    rows, d = dy_ref.shape
    ff = gate_ref.shape[1]
    half, cols = rows // 2, d // 2
    ring = side - 1
    slots = side * side - 1
    me = lax.axis_index("tp")
    at = (me // side, me % side)

    def owner(da, db):
        return lax.rem(at[0] + da + 2 * side, side) * side + lax.rem(at[1] + db + 2 * side, side)

    def on_link(link, along, across):
        axis, sign = link
        steps = (sign * along, sign * across)
        return owner(*(steps if axis == 0 else steps[::-1]))

    def unit(link, slot, back):
        array, s = slot // slots, slot % slots
        early = s < 2 * ring
        late = jnp.maximum(s - 2 * ring, 0)
        hop = jnp.where(early, s // 2, late // ring) + 1
        across = jnp.where(early, 0, late % ring + 1)
        second = jnp.where(early, s % 2, 1)
        who = on_link(link, back - hop, -across)
        axis, sign = link
        col = second if axis == 0 else 1 - second
        row = pl.multiple_of(who * rows + (0 if sign == 1 else half), 8)
        return full_ref.at[array, pl.ds(row, half), pl.ds(pl.multiple_of(col * cols, 128), cols)]

    def copy(k, slot, src, dst):
        return pltpu.make_async_remote_copy(
            src_ref=src,
            dst_ref=dst,
            send_sem=send_sem.at[k, slot],
            recv_sem=recv_sem.at[k, slot],
            device_id={"tp": on_link(LINKS[k], 1, 0)},
            device_id_type=MESH,
        )

    def send(slot):
        for k, link in enumerate(LINKS):
            part = unit(link, slot, 1)
            copy(k, slot, part, part).start()

    def arrive(slot):
        for k, link in enumerate(LINKS):
            part = unit(link, slot, 0)
            copy(k, slot, part, part).wait_recv()

    def step(slot):
        arrive(slot)

        @pl.when(slot + 2 < 2 * slots)
        def _():
            send(slot + 2)

    barrier = pltpu.get_barrier_semaphore()
    for link in LINKS:
        pl.semaphore_signal(barrier, inc=1, device_id={"tp": on_link(link, 1, 0)}, device_id_type=MESH)
    pl.semaphore_wait(barrier, len(LINKS))

    for slot in range(2):
        for k, (axis, sign) in enumerate(LINKS):
            col = slot if axis == 0 else 1 - slot
            r = 0 if sign == 1 else half
            part = (pl.ds(r, half), pl.ds(col * cols, cols))
            row = pl.multiple_of(me * rows + r, 8)
            copy(k, slot, dy_ref.at[part], full_ref.at[0, pl.ds(row, half), part[1]]).start()

    wd_copy = pltpu.make_async_copy(wd_ref, wd_v, wd_sem)
    wd_copy.start()

    mine = pl.ds(pl.multiple_of(me * rows, 8), rows)
    own = [dy_v.at[pl.ds(i * rows, rows)] for i in range(2)]
    loads = [pltpu.make_async_copy(ref, own[i], in_sem.at[0, i]) for i, ref in enumerate((dy_ref, x_ref))]
    stores = [pltpu.make_async_copy(own[i], full_ref.at[i, mine], in_sem.at[1, i]) for i in range(2)]
    for load in loads:
        load.start()
    for load, store in zip(loads, stores):
        load.wait()
        store.start()
    for store in stores:
        store.wait()

    tiles = d // dt
    cut = tiles // 2

    count = side * (side // 2) * tiles

    def weights(i, slot):
        part = pl.ds(pl.multiple_of(i * dt, dt), dt)
        return [
            pltpu.make_async_copy(ref.at[part], buf.at[slot], w_sem.at[j, slot])
            for j, (ref, buf) in enumerate(((wg_ref, wg_t), (wu_ref, wu_t)))
        ]

    for i in range(DEPTH - 1):
        for c in weights(i % tiles, i):
            c.start()
    lax.fori_loop(0, FIRST, lambda s, _: (step(s), None)[1], None)
    wd_copy.wait()

    local = [pl.ds(i * half, half) for i in range(4)]

    def rows_of(q, p):
        starts = []
        for a in (2 * p, 2 * p + 1):
            starts += [owner(-a, -q) * rows, owner(a, q) * rows + half]
        return [pl.ds(pl.multiple_of(s, 8), half) for s in starts]

    def reads(q, p):
        return [
            pltpu.make_async_copy(ref.at[t], buf.at[h], in_sem.at[j, i])
            for j, (ref, buf) in enumerate(((full_ref.at[0], dy_v), (gate_ref, g_v), (up_ref, u_v)))
            for i, (t, h) in enumerate(zip(rows_of(q, p), local))
        ]

    def group(q, p):
        offsets = [2 * p, 2 * p + 1]
        there = rows_of(q, p)
        which = q * (side // 2) + p
        first = FIRST + TICKS * which

        step(first)
        for c in reads(q, p):
            c.wait()

        def hidden_tile(i, _):
            n = pl.ds(pl.multiple_of(i * nt, nt), nt)
            d_hidden = lax.dot_general(
                dy_v[...], wd_v[n, :], (((1,), (1,)), ((), ())), preferred_element_type=jnp.float32
            )
            gate, up = g_v[:, n].astype(jnp.float32), u_v[:, n].astype(jnp.float32)
            s = jax.nn.sigmoid(gate)
            silu = gate * s
            d_silu = d_hidden * up
            dg_v[:, n] = (d_silu * s + d_silu * gate * (s * (1 - s))).astype(dg_v.dtype)
            du_v[:, n] = (d_hidden * silu).astype(du_v.dtype)
            h_v[:, n] = (silu * up).astype(h_v.dtype)

        lax.fori_loop(0, ff // nt, hidden_tile, None)
        results = [
            pltpu.make_async_copy(buf.at[h], ref.at[t, c], res_sem.at[j, i])
            for j, (buf, ref, c) in enumerate((
                (dg_v, dgu_ref, pl.ds(0, ff)), (du_v, dgu_ref, pl.ds(ff, ff)), (h_v, hid_ref, pl.ds(0, ff)),
            ))
            for i, (t, h) in enumerate(zip(there, local))
        ]
        for c in results:
            c.start()
        step(first + 1)

        @pl.when(which + 1 < side * (side // 2))
        def _():
            for c in reads(q + (p + 1) // (side // 2), (p + 1) % (side // 2)):
                c.start()

        def stores_of(i, slot, second, b):
            n = pl.ds(pl.multiple_of((i - second * cut) * dt, dt), dt)
            copies = []
            for j, a in enumerate(offsets):
                for r in range(2):
                    da, db = ((-a) % side, (side - b) % side) if r == 0 else (a, b)
                    key, at_ = (2 * side + 2 * db + r, da) if second else (2 * da + r, db)
                    k = 2 * j + r
                    copies.append(pltpu.make_async_copy(
                        out_t.at[slot, local[k]], terms[key].at[at_, :, n], out_sem.at[slot, k]
                    ))
            return copies

        def for_stores(i, slot, second, act):
            if not second:
                for c in stores_of(i, slot, second, q):
                    act(c)
                return
            for b in range(side):

                @pl.when(q == b)
                def _():
                    for c in stores_of(i, slot, second, b):
                        act(c)

        def dx_tile(second):
            begin = cut if second else 0

            def body(i, _):
                at_ = which * tiles + i
                slot = at_ % DEPTH
                for c in weights(i, slot):
                    c.wait()

                @pl.when(at_ + DEPTH - 1 < count)
                def _():
                    for c in weights((i + DEPTH - 1) % tiles, (at_ + DEPTH - 1) % DEPTH):
                        c.start()

                @pl.when(at_ >= DEPTH)
                def _():
                    for c in stores_of(0, slot, False, q):
                        c.wait()

                nt_dims = (((1,), (1,)), ((), ()))
                term = lax.dot_general(dg_v[...], wg_t[slot], nt_dims, preferred_element_type=jnp.float32)
                term += lax.dot_general(du_v[...], wu_t[slot], nt_dims, preferred_element_type=jnp.float32)
                out_t[slot] = term.astype(out_t.dtype)
                for_stores(i, slot, second, lambda c: c.start())

            lax.fori_loop(begin, tiles if second else cut, body, None)

        dx_tile(False)
        dx_tile(True)
        for c in results:
            c.wait()

        if p == side // 2 - 1:

            @pl.when(q == side - 1)
            def _():
                for slot in range(DEPTH):
                    for c in stores_of(0, slot, False, q):
                        c.wait()

    def groups(q, _):
        for p in range(side // 2):
            group(q, p)

    for c in reads(0, 0):
        c.start()
    lax.fori_loop(0, side, groups, None)
    done = FIRST + TICKS * side * (side // 2)

    fm = ff // 2
    tokens = hid_ref.shape[0]
    tb = tile_of(tokens, 512)
    per = -(-tiles // PARTS)

    def dy_tile(i, slot):
        n = pl.ds(pl.multiple_of(i * dt, dt), dt)
        return pltpu.make_async_copy(full_ref.at[0, :, n], dy_t.at[slot], dyt_sem.at[slot])

    def dwd_tile(m, i, slot):
        n = pl.ds(pl.multiple_of(i * dt, dt), dt)
        row = pl.ds(pl.multiple_of(m * fm, fm), fm)
        return pltpu.make_async_copy(dwd_t.at[slot], dwd_ref.at[row, n], dwd_sem.at[slot])

    for i in range(DEEP - 1):
        dy_tile(i % tiles, i).start()

    def down(m, _):
        load = pltpu.make_async_copy(hid_ref.at[:, pl.ds(pl.multiple_of(m * fm, fm), fm)], hid_v, hid_sem)
        load.start()
        load.wait()
        for b in range(tokens // tb):
            ht_v[:, b * tb : (b + 1) * tb] = hid_v[b * tb : (b + 1) * tb, :].T

        def tile(i, _):
            at_ = m * tiles + i
            slot = at_ % DEEP
            dy_tile(i, slot).wait()

            @pl.when(at_ + DEEP - 1 < 2 * tiles)
            def _():
                dy_tile((i + DEEP - 1) % tiles, (at_ + DEEP - 1) % DEEP).start()

            @pl.when(at_ >= DEEP)
            def _():
                dwd_tile(m, i, slot).wait()

            dw = jnp.dot(ht_v[...], dy_t[slot], preferred_element_type=jnp.float32)
            dwd_t[slot] = dw.astype(dwd_t.dtype)
            dwd_tile(m, i, slot).start()

        def part(k, _):
            step(done + m * PARTS + k)
            lax.fori_loop(k * per, jnp.minimum((k + 1) * per, tiles), tile, None)

        lax.fori_loop(0, PARTS, part, None)

    lax.fori_loop(0, 2, down, None)
    for slot in range(DEEP):
        dwd_tile(1, 0, slot).wait()
    lax.fori_loop(done + 2 * PARTS, 2 * slots, lambda s, _: (step(s), None)[1], None)

    def sent(slot, _):
        for k, link in enumerate(LINKS):
            part = unit(link, slot, 1)
            copy(k, slot, part, part).wait_send()

    lax.fori_loop(0, 2 * slots, sent, None)


def gather(side, x, dy, gate, up, wg, wu, wd):
    rows, d = dy.shape
    tokens, ff = gate.shape
    n = side * side
    group = 2 * rows
    dt, nt = tile_of(d // 2, 512), tile_of(ff, 256)
    bf16 = jnp.bfloat16
    flops = 8 * tokens * d * ff
    anywhere = pl.BlockSpec(memory_space=pltpu.HBM)
    return pl.pallas_call(
        functools.partial(gather_kernel, side, dt, nt),
        out_shape=(
            jax.ShapeDtypeStruct((2, tokens, d), bf16),
            jax.ShapeDtypeStruct((tokens, 2 * ff), bf16),
            jax.ShapeDtypeStruct((tokens, ff), bf16),
            jax.ShapeDtypeStruct((ff, d), bf16),
            *[jax.ShapeDtypeStruct((side, rows // 2, d // 2), bf16)] * (4 * side),
        ),
        in_specs=[anywhere] * 7,
        out_specs=(anywhere,) * (4 + 4 * side),
        scratch_shapes=[
            pltpu.VMEM((ff, d), bf16),
            pltpu.VMEM((group, d), bf16),
            *[pltpu.VMEM((group, ff), bf16)] * 5,
            *[pltpu.VMEM((DEPTH, dt, ff), bf16)] * 2,
            pltpu.VMEM((DEPTH, group, dt), bf16),
            pltpu.VMEM((tokens, ff // 2), bf16),
            pltpu.VMEM((ff // 2, tokens), bf16),
            pltpu.VMEM((DEEP, tokens, dt), bf16),
            pltpu.VMEM((DEEP, ff // 2, dt), bf16),
            pltpu.SemaphoreType.DMA((len(LINKS), 2 * (n - 1))),
            pltpu.SemaphoreType.DMA((len(LINKS), 2 * (n - 1))),
            pltpu.SemaphoreType.DMA,
            pltpu.SemaphoreType.DMA((3, 4)),
            pltpu.SemaphoreType.DMA((3, 4)),
            pltpu.SemaphoreType.DMA((2, DEPTH)),
            pltpu.SemaphoreType.DMA((DEPTH, 4)),
            pltpu.SemaphoreType.DMA,
            pltpu.SemaphoreType.DMA((DEEP,)),
            pltpu.SemaphoreType.DMA((DEEP,)),
        ],
        compiler_params=pltpu.CompilerParams(
            collective_id=0, has_side_effects=True, vmem_limit_bytes=VMEM
        ),
        cost_estimate=pl.CostEstimate(
            flops=flops, bytes_accessed=2 * (8 * 2 * d * ff + 6 * tokens * d), transcendentals=tokens * ff
        ),
        name="gather_and_dx",
    )(x, dy, gate, up, wg, wu, wd)


def dw_in_kernel(sums, moved, *refs):
    x_ref, d_ref, *rest = refs
    outs = rest[len(rest) - 2 - 2 * sums - moved :]
    dwg_ref, dwu_ref = outs[:2]
    ff = dwg_ref.shape[1]
    dw = lax.dot_general(
        x_ref[...], d_ref[...], (((0,), (0,)), ((), ())), preferred_element_type=jnp.float32
    )
    dwg_ref[...] = dw[:, :ff].astype(dwg_ref.dtype)
    dwu_ref[...] = dw[:, ff:].astype(dwu_ref.dtype)
    for k in range(sums):
        mine, came = rest[2 * k : 2 * k + 2]
        total = bf16(f32(mine[...]) + f32(came[...]))
        outs[2 + 2 * k][...] = total[:1]
        outs[3 + 2 * k][...] = total[1:]
    for k in range(moved):
        outs[2 + 2 * sums + k][...] = rest[2 * sums + k][...]


def dw_in(full, dgu, first, last, so_far=(), pairs=(), moved=()):
    _, tokens, d = full.shape
    ff = dgu.shape[1] // 2
    bd = tile_of(d, 256)
    n = last - first
    flat = [v for pair in pairs for v in pair]
    resident = 2 * dgu.size

    def along(v):
        lead = v.shape[:-1]
        return pl.BlockSpec((*lead, v.shape[-1] // n), lambda i: (*[0] * len(lead), i))

    cut = [jax.ShapeDtypeStruct((k, *a.shape[1:]), a.dtype) for a, _ in pairs for k in (1, a.shape[0] - 1)]
    extra = [*cut, *moved]
    new = [jax.ShapeDtypeStruct((d, ff), full.dtype)] * 2 + [jax.ShapeDtypeStruct(v.shape, v.dtype) for v in extra]
    return pl.pallas_call(
        functools.partial(dw_in_kernel, len(pairs), len(moved)),
        grid=(n,),
        out_shape=new,
        in_specs=[
            pl.BlockSpec((pl.squeezed, tokens, bd), lambda i: (1, 0, i + first)),
            pl.BlockSpec(memory_space=pltpu.VMEM),
            *[along(v) for v in (*flat, *moved)],
            *[pl.BlockSpec(memory_space=pltpu.HBM)] * len(so_far),
        ],
        out_specs=[*[pl.BlockSpec((bd, ff), lambda i: (i + first, 0))] * 2, *[along(v) for v in extra]],
        input_output_aliases={2 + len(flat) + len(moved) + i: i for i in range(len(so_far))},
        compiler_params=pltpu.CompilerParams(vmem_limit_bytes=VMEM - resident - 65536),
        cost_estimate=pl.CostEstimate(
            flops=4 * tokens * n * bd * ff, bytes_accessed=2 * (tokens * n * bd + 2 * ff * (tokens + n * bd)), transcendentals=0
        ),
        name="dw_in",
    )(full, dgu, *flat, *moved, *so_far)


def f32(v):
    return v.astype(jnp.float32)


def bf16(v):
    return v.astype(jnp.bfloat16)


def finish_kernel(side, *refs):
    ins, own, rest = refs[:12], refs[12:16], refs[16:]
    sum_ref, came_ref, in_v, send_v, recv_v, own_v, in_sem, send_sem, recv_sem, own_send, own_recv = rest
    me = lax.axis_index("tp")
    at = (me // side, me % side)

    def neighbour(axis, sign):
        to = [at[0], at[1]]
        to[axis] = lax.rem(to[axis] + sign + side, side)
        return {"tp": to[0] * side + to[1]}

    barrier = pltpu.get_barrier_semaphore()
    for axis, sign in LINKS:
        pl.semaphore_signal(barrier, inc=1, device_id=neighbour(axis, sign), device_id_type=MESH)

    order = (((2, 0), (2, 1)), ((1, 1), (3, 0)), ((1, 0), (3, 1)))

    def loads(h, j, r):
        copies = []
        for k in range(3):
            late = k == 1 + r
            if late and j == 0:
                continue
            src = ins[6 * h + 3 * r + k].at[j - 1 if late else j]
            copies.append(pltpu.make_async_copy(src, in_v.at[h, j, r, k], in_sem.at[h, j, r, k]))
        return copies

    def own_message(h, way):
        return pltpu.make_async_remote_copy(
            src_ref=own[2 * h + way].at[0],
            dst_ref=own_v.at[h, way],
            send_sem=own_send.at[h, way],
            recv_sem=own_recv.at[h, way],
            device_id=neighbour(h, 1 - 2 * way),
            device_id_type=MESH,
        )

    def message(h, step, way):
        return pltpu.make_async_remote_copy(
            src_ref=send_v.at[h, step, way],
            dst_ref=recv_v.at[h, way] if step == 0 else came_ref.at[h, step - 1, way],
            send_sem=send_sem.at[h, step, way],
            recv_sem=recv_sem.at[h, step, way],
            device_id=neighbour(1 - h, 1 - 2 * way),
            device_id_type=MESH,
        )

    def piece(h, j, r):
        for c in loads(h, j, r):
            c.wait()
        total = f32(in_v[h, j, r, 0])
        for k in (1, 2):
            if k == 1 + r and j == 0:
                own_message(h, r).wait_recv()
                total += f32(own_v[h, r])
            else:
                total += f32(in_v[h, j, r, k])
        return total

    pieces = [p for step in order for p in step] + [(0, 0), (0, 1)]
    for j, r in pieces:
        for h in range(2):
            for c in loads(h, j, r):
                c.start()
    pl.semaphore_wait(barrier, len(LINKS))
    for h in range(2):
        for way in range(2):
            own_message(h, way).start()
    for step, steps in enumerate(order):
        for h in range(2):
            for way, (j, r) in enumerate(steps):
                total = piece(h, j, r)
                if step == 2:
                    message(h, 0, way).wait_recv()
                    total += f32(recv_v[h, way])
                send_v[h, step, way] = bf16(total)
                message(h, step, way).start()
    for h in range(2):
        for r in range(2):
            sum_ref[h, r] = piece(h, 0, r)
    for step in (1, 2):
        for h in range(2):
            for way in range(2):
                message(h, step, way).wait_recv()
    for h in range(2):
        for way in range(2):
            own_message(h, way).wait_send()
            for step in range(3):
                message(h, step, way).wait_send()


def finish(side, ins, own):
    _, half, cols = ins[0].shape
    hbm, vmem = pl.BlockSpec(memory_space=pltpu.HBM), pl.BlockSpec(memory_space=pltpu.VMEM)
    dtype = jnp.bfloat16
    mine, came = pl.pallas_call(
        functools.partial(finish_kernel, side),
        out_shape=(pltpu.VMEM((2, 2, half, cols), jnp.float32), pltpu.VMEM((2, 2, 2, half, cols), dtype)),
        in_specs=[hbm] * (len(ins) + len(own)),
        out_specs=(vmem, vmem),
        scratch_shapes=[
            pltpu.VMEM((2, side, 2, 3, half, cols), dtype),
            pltpu.VMEM((2, 3, 2, half, cols), dtype),
            pltpu.VMEM((2, 2, half, cols), dtype),
            pltpu.VMEM((2, 2, half, cols), dtype),
            pltpu.SemaphoreType.DMA((2, side, 2, 3)),
            pltpu.SemaphoreType.DMA((2, 3, 2)),
            pltpu.SemaphoreType.DMA((2, 3, 2)),
            pltpu.SemaphoreType.DMA((2, 2)),
            pltpu.SemaphoreType.DMA((2, 2)),
        ],
        compiler_params=pltpu.CompilerParams(
            collective_id=1, has_side_effects=True, vmem_limit_bytes=FINISH
        ),
        cost_estimate=pl.CostEstimate(
            flops=64 * half * cols, bytes_accessed=2 * 52 * half * cols, transcendentals=0
        ),
        name="finish_dx",
    )(*ins, *own)

    chunk = tile_of(cols, cols // 2)

    def last_sum(mine_ref, came_ref, out_ref):
        i = pl.program_id(0)
        h, c = i // 2, pl.ds(pl.multiple_of(i % 2 * chunk, 128), chunk)
        for r in range(2):
            total = mine_ref[h, r, :, c] + f32(came_ref[h, 0, 1 - r, :, c]) + f32(came_ref[h, 1, r, :, c])
            out_ref[r * half : (r + 1) * half, :] = bf16(total)

    return pl.pallas_call(
        last_sum,
        grid=(4,),
        out_shape=jax.ShapeDtypeStruct((2 * half, 2 * cols), dtype),
        in_specs=[vmem, vmem],
        out_specs=pl.BlockSpec((2 * half, chunk), lambda i: (0, i)),
        compiler_params=pltpu.CompilerParams(vmem_limit_bytes=16 * 1024 * 1024),
        cost_estimate=pl.CostEstimate(flops=8 * half * cols, bytes_accessed=16 * half * cols, transcendentals=0),
        name="last_sum",
    )(mine, came)


def solution(mesh):
    side = math.isqrt(mesh.shape["tp"])

    def hop(v, axis, sign):
        pairs = []
        for i in range(side * side):
            at = [i // side, i % side]
            at[axis] = (at[axis] + sign) % side
            pairs.append((i, at[0] * side + at[1]))
        return lax.ppermute(v, "tp", pairs)

    def device_step(x, dy, gate, up, w_gate, w_up, w_down):
        full, dgu, _, dw_down, *terms = gather(side, x, dy, gate, up, w_gate, w_up, w_down)
        t = [[terms[2 * (h * side + k) :][:2] for k in range(side)] for h in range(2)]
        dgu = pltpu.with_memory_space_constraint(dgu, pltpu.VMEM)
        blocks = x.shape[1] // tile_of(x.shape[1], 256)
        cuts = [0, blocks * 14 // 28, blocks * 18 // 28, blocks]
        far = [(hop(v[2][0], h, 1), hop(v[2][1], h, -1)) for h, v in enumerate(t)]
        raw = [(hop(v[1][1], h, 1), hop(v[3][0], h, -1)) for h, v in enumerate(t)]
        *dw, dw_down = dw_in(full, dgu, cuts[0], cuts[1], moved=[dw_down])
        pairs = [(v[1][0], f[0]) for v, f in zip(t, far)] + [(v[3][1], f[1]) for v, f in zip(t, far)]
        *dw, a0, a, b0, b, c0, c, d0, d = dw_in(full, dgu, cuts[1], cuts[2], dw, pairs)
        near = [(hop(up_, h, 1), hop(down, h, -1)) for h, (up_, down) in enumerate(((a, c), (b, d)))]
        dw = dw_in(full, dgu, cuts[2], cuts[3], dw)
        ins = []
        for v, r, n in zip(t, raw, near):
            ins += [v[0][0], n[0], r[1], v[0][1], r[0], n[1]]
        dx = finish(side, ins, [a0, c0, b0, d0])
        return dx, *dw, dw_down

    rows, both, cols = P(("dp", "tp"), None), P("dp", "tp"), P(None, "tp")
    return jax.shard_map(
        device_step,
        mesh=mesh,
        in_specs=(rows, rows, both, both, cols, cols, P("tp", None)),
        out_specs=(rows, both, both, rows),
        check_vma=False,
    )
```

```python
import functools
import math

import jax
import jax.numpy as jnp
from jax import lax
from jax.experimental import pallas as pl
from jax.experimental.pallas import tpu as pltpu
from jax.sharding import PartitionSpec as P

MESH = pl.DeviceIdType.MESH
LINKS = ((0, 1), (0, -1), (1, 1), (1, -1))
TICKS = 2
FIRST = 7
VMEM = 65400 * 1024
FINISH = 54 * 1024 * 1024
DEPTH = 4
DEEP = 3
PARTS = 3


def tile_of(size, want):
    return want if size % want == 0 else size


def gather_kernel(
    side, dt, nt,
    x_ref, dy_ref, gate_ref, up_ref, wg_ref, wu_ref, wd_ref,
    full_ref, dgu_ref, hid_ref, dwd_ref, *rest,
):
    terms, scratch = rest[: 4 * side], rest[4 * side :]
    (
    wd_v, dy_v, g_v, u_v, dg_v, du_v, h_v, wg_t, wu_t, out_t, hid_v, ht_v, dy_t, dwd_t,
    send_sem, recv_sem, wd_sem, in_sem, res_sem, w_sem, out_sem, hid_sem, dyt_sem, dwd_sem,
    ) = scratch
    rows, d = dy_ref.shape
    ff = gate_ref.shape[1]
    half, cols = rows // 2, d // 2
    ring = side - 1
    slots = side * side - 1
    me = lax.axis_index("tp")
    at = (me // side, me % side)

    def owner(da, db):
        return lax.rem(at[0] + da + 2 * side, side) * side + lax.rem(at[1] + db + 2 * side, side)

    def on_link(link, along, across):
        axis, sign = link
        steps = (sign * along, sign * across)
        return owner(*(steps if axis == 0 else steps[::-1]))

    def unit(link, slot, back):
        array, s = slot // slots, slot % slots
        early = s < 2 * ring
        late = jnp.maximum(s - 2 * ring, 0)
        hop = jnp.where(early, s // 2, late // ring) + 1
        across = jnp.where(early, 0, late % ring + 1)
        second = jnp.where(early, s % 2, 1)
        who = on_link(link, back - hop, -across)
        axis, sign = link
        col = second if axis == 0 else 1 - second
        row = pl.multiple_of(who * rows + (0 if sign == 1 else half), 8)
        return full_ref.at[array, pl.ds(row, half), pl.ds(pl.multiple_of(col * cols, 128), cols)]

    def copy(k, slot, src, dst):
        return pltpu.make_async_remote_copy(
            src_ref=src,
            dst_ref=dst,
            send_sem=send_sem.at[k, slot],
            recv_sem=recv_sem.at[k, slot],
            device_id={"tp": on_link(LINKS[k], 1, 0)},
            device_id_type=MESH,
        )

    def send(slot):
        for k, link in enumerate(LINKS):
            part = unit(link, slot, 1)
            copy(k, slot, part, part).start()

    def arrive(slot):
        for k, link in enumerate(LINKS):
            part = unit(link, slot, 0)
            copy(k, slot, part, part).wait_recv()

    def step(slot):
        arrive(slot)

        @pl.when(slot + 2 < 2 * slots)
        def _():
            send(slot + 2)

    barrier = pltpu.get_barrier_semaphore()
    for link in LINKS:
        pl.semaphore_signal(barrier, inc=1, device_id={"tp": on_link(link, 1, 0)}, device_id_type=MESH)
    pl.semaphore_wait(barrier, len(LINKS))

    for slot in range(2):
        for k, (axis, sign) in enumerate(LINKS):
            col = slot if axis == 0 else 1 - slot
            r = 0 if sign == 1 else half
            part = (pl.ds(r, half), pl.ds(col * cols, cols))
            row = pl.multiple_of(me * rows + r, 8)
            copy(k, slot, dy_ref.at[part], full_ref.at[0, pl.ds(row, half), part[1]]).start()

    wd_copy = pltpu.make_async_copy(wd_ref, wd_v, wd_sem)
    wd_copy.start()

    mine = pl.ds(pl.multiple_of(me * rows, 8), rows)
    own = [dy_v.at[pl.ds(i * rows, rows)] for i in range(2)]
    loads = [pltpu.make_async_copy(ref, own[i], in_sem.at[0, i]) for i, ref in enumerate((dy_ref, x_ref))]
    stores = [pltpu.make_async_copy(own[i], full_ref.at[i, mine], in_sem.at[1, i]) for i in range(2)]
    for load in loads:
        load.start()
    for load, store in zip(loads, stores):
        load.wait()
        store.start()
    for store in stores:
        store.wait()

    tiles = d // dt
    cut = tiles // 2

    count = side * (side // 2) * tiles

    def weights(i, slot):
        part = pl.ds(pl.multiple_of(i * dt, dt), dt)
        return [
            pltpu.make_async_copy(ref.at[part], buf.at[slot], w_sem.at[j, slot])
            for j, (ref, buf) in enumerate(((wg_ref, wg_t), (wu_ref, wu_t)))
        ]

    for i in range(DEPTH - 1):
        for c in weights(i % tiles, i):
            c.start()
    lax.fori_loop(0, FIRST, lambda s, _: (step(s), None)[1], None)
    wd_copy.wait()

    local = [pl.ds(i * half, half) for i in range(4)]

    def rows_of(q, p):
        starts = []
        for a in (2 * p, 2 * p + 1):
            starts += [owner(-a, -q) * rows, owner(a, q) * rows + half]
        return [pl.ds(pl.multiple_of(s, 8), half) for s in starts]

    def reads(q, p):
        return [
            pltpu.make_async_copy(ref.at[t], buf.at[h], in_sem.at[j, i])
            for j, (ref, buf) in enumerate(((full_ref.at[0], dy_v), (gate_ref, g_v), (up_ref, u_v)))
            for i, (t, h) in enumerate(zip(rows_of(q, p), local))
        ]

    def group(q, p):
        offsets = [2 * p, 2 * p + 1]
        there = rows_of(q, p)
        which = q * (side // 2) + p
        first = FIRST + TICKS * which

        step(first)
        for c in reads(q, p):
            c.wait()

        def hidden_tile(i, _):
            n = pl.ds(pl.multiple_of(i * nt, nt), nt)
            d_hidden = lax.dot_general(
                dy_v[...], wd_v[n, :], (((1,), (1,)), ((), ())), preferred_element_type=jnp.float32
            )
            gate, up = g_v[:, n].astype(jnp.float32), u_v[:, n].astype(jnp.float32)
            s = jax.nn.sigmoid(gate)
            silu = gate * s
            d_silu = d_hidden * up
            dg_v[:, n] = (d_silu * s + d_silu * gate * (s * (1 - s))).astype(dg_v.dtype)
            du_v[:, n] = (d_hidden * silu).astype(du_v.dtype)
            h_v[:, n] = (silu * up).astype(h_v.dtype)

        lax.fori_loop(0, ff // nt, hidden_tile, None)
        results = [
            pltpu.make_async_copy(buf.at[h], ref.at[t, c], res_sem.at[j, i])
            for j, (buf, ref, c) in enumerate((
                (dg_v, dgu_ref, pl.ds(0, ff)), (du_v, dgu_ref, pl.ds(ff, ff)), (h_v, hid_ref, pl.ds(0, ff)),
            ))
            for i, (t, h) in enumerate(zip(there, local))
        ]
        for c in results:
            c.start()
        step(first + 1)

        @pl.when(which + 1 < side * (side // 2))
        def _():
            for c in reads(q + (p + 1) // (side // 2), (p + 1) % (side // 2)):
                c.start()

        def stores_of(i, slot, second, b):
            n = pl.ds(pl.multiple_of((i - second * cut) * dt, dt), dt)
            copies = []
            for j, a in enumerate(offsets):
                for r in range(2):
                    da, db = ((-a) % side, (side - b) % side) if r == 0 else (a, b)
                    key, at_ = (2 * side + 2 * db + r, da) if second else (2 * da + r, db)
                    k = 2 * j + r
                    copies.append(pltpu.make_async_copy(
                        out_t.at[slot, local[k]], terms[key].at[at_, :, n], out_sem.at[slot, k]
                    ))
            return copies

        def for_stores(i, slot, second, act):
            if not second:
                for c in stores_of(i, slot, second, q):
                    act(c)
                return
            for b in range(side):

                @pl.when(q == b)
                def _():
                    for c in stores_of(i, slot, second, b):
                        act(c)

        def dx_tile(second):
            begin = cut if second else 0

            def body(i, _):
                at_ = which * tiles + i
                slot = at_ % DEPTH
                for c in weights(i, slot):
                    c.wait()

                @pl.when(at_ + DEPTH - 1 < count)
                def _():
                    for c in weights((i + DEPTH - 1) % tiles, (at_ + DEPTH - 1) % DEPTH):
                        c.start()

                @pl.when(at_ >= DEPTH)
                def _():
                    for c in stores_of(0, slot, False, q):
                        c.wait()

                nt_dims = (((1,), (1,)), ((), ()))
                term = lax.dot_general(dg_v[...], wg_t[slot], nt_dims, preferred_element_type=jnp.float32)
                term += lax.dot_general(du_v[...], wu_t[slot], nt_dims, preferred_element_type=jnp.float32)
                out_t[slot] = term.astype(out_t.dtype)
                for_stores(i, slot, second, lambda c: c.start())

            lax.fori_loop(begin, tiles if second else cut, body, None)

        dx_tile(False)
        dx_tile(True)
        for c in results:
            c.wait()

        if p == side // 2 - 1:

            @pl.when(q == side - 1)
            def _():
                for slot in range(DEPTH):
                    for c in stores_of(0, slot, False, q):
                        c.wait()

    def groups(q, _):
        for p in range(side // 2):
            group(q, p)

    for c in reads(0, 0):
        c.start()
    lax.fori_loop(0, side, groups, None)
    done = FIRST + TICKS * side * (side // 2)

    fm = ff // 2
    tokens = hid_ref.shape[0]
    tb = tile_of(tokens, 512)
    per = -(-tiles // PARTS)

    def dy_tile(i, slot):
        n = pl.ds(pl.multiple_of(i * dt, dt), dt)
        return pltpu.make_async_copy(full_ref.at[0, :, n], dy_t.at[slot], dyt_sem.at[slot])

    def dwd_tile(m, i, slot):
        n = pl.ds(pl.multiple_of(i * dt, dt), dt)
        row = pl.ds(pl.multiple_of(m * fm, fm), fm)
        return pltpu.make_async_copy(dwd_t.at[slot], dwd_ref.at[row, n], dwd_sem.at[slot])

    for i in range(DEEP - 1):
        dy_tile(i % tiles, i).start()

    def down(m, _):
        load = pltpu.make_async_copy(hid_ref.at[:, pl.ds(pl.multiple_of(m * fm, fm), fm)], hid_v, hid_sem)
        load.start()
        load.wait()
        for b in range(tokens // tb):
            ht_v[:, b * tb : (b + 1) * tb] = hid_v[b * tb : (b + 1) * tb, :].T

        def tile(i, _):
            at_ = m * tiles + i
            slot = at_ % DEEP
            dy_tile(i, slot).wait()

            @pl.when(at_ + DEEP - 1 < 2 * tiles)
            def _():
                dy_tile((i + DEEP - 1) % tiles, (at_ + DEEP - 1) % DEEP).start()

            @pl.when(at_ >= DEEP)
            def _():
                dwd_tile(m, i, slot).wait()

            dw = jnp.dot(ht_v[...], dy_t[slot], preferred_element_type=jnp.float32)
            dwd_t[slot] = dw.astype(dwd_t.dtype)
            dwd_tile(m, i, slot).start()

        def part(k, _):
            step(done + m * PARTS + k)
            lax.fori_loop(k * per, jnp.minimum((k + 1) * per, tiles), tile, None)

        lax.fori_loop(0, PARTS, part, None)

    lax.fori_loop(0, 2, down, None)
    for slot in range(DEEP):
        dwd_tile(1, 0, slot).wait()
    lax.fori_loop(done + 2 * PARTS, 2 * slots, lambda s, _: (step(s), None)[1], None)

    def sent(slot, _):
        for k, link in enumerate(LINKS):
            part = unit(link, slot, 1)
            copy(k, slot, part, part).wait_send()

    lax.fori_loop(0, 2 * slots, sent, None)


def gather(side, x, dy, gate, up, wg, wu, wd):
    rows, d = dy.shape
    tokens, ff = gate.shape
    n = side * side
    group = 2 * rows
    dt, nt = tile_of(d // 2, 512), tile_of(ff, 256)
    bf16 = jnp.bfloat16
    flops = 8 * tokens * d * ff
    anywhere = pl.BlockSpec(memory_space=pltpu.HBM)
    return pl.pallas_call(
        functools.partial(gather_kernel, side, dt, nt),
        out_shape=(
            jax.ShapeDtypeStruct((2, tokens, d), bf16),
            jax.ShapeDtypeStruct((tokens, 2 * ff), bf16),
            jax.ShapeDtypeStruct((tokens, ff), bf16),
            jax.ShapeDtypeStruct((ff, d), bf16),
            *[jax.ShapeDtypeStruct((side, rows // 2, d // 2), bf16)] * (4 * side),
        ),
        in_specs=[anywhere] * 7,
        out_specs=(anywhere,) * (4 + 4 * side),
        scratch_shapes=[
            pltpu.VMEM((ff, d), bf16),
            pltpu.VMEM((group, d), bf16),
            *[pltpu.VMEM((group, ff), bf16)] * 5,
            *[pltpu.VMEM((DEPTH, dt, ff), bf16)] * 2,
            pltpu.VMEM((DEPTH, group, dt), bf16),
            pltpu.VMEM((tokens, ff // 2), bf16),
            pltpu.VMEM((ff // 2, tokens), bf16),
            pltpu.VMEM((DEEP, tokens, dt), bf16),
            pltpu.VMEM((DEEP, ff // 2, dt), bf16),
            pltpu.SemaphoreType.DMA((len(LINKS), 2 * (n - 1))),
            pltpu.SemaphoreType.DMA((len(LINKS), 2 * (n - 1))),
            pltpu.SemaphoreType.DMA,
            pltpu.SemaphoreType.DMA((3, 4)),
            pltpu.SemaphoreType.DMA((3, 4)),
            pltpu.SemaphoreType.DMA((2, DEPTH)),
            pltpu.SemaphoreType.DMA((DEPTH, 4)),
            pltpu.SemaphoreType.DMA,
            pltpu.SemaphoreType.DMA((DEEP,)),
            pltpu.SemaphoreType.DMA((DEEP,)),
        ],
        compiler_params=pltpu.CompilerParams(
            collective_id=0, has_side_effects=True, vmem_limit_bytes=VMEM
        ),
        cost_estimate=pl.CostEstimate(
            flops=flops, bytes_accessed=2 * (8 * 2 * d * ff + 6 * tokens * d), transcendentals=tokens * ff
        ),
        name="gather_and_dx",
    )(x, dy, gate, up, wg, wu, wd)


def dw_in_kernel(sums, moved, *refs):
    x_ref, d_ref, *rest = refs
    outs = rest[len(rest) - 2 - 2 * sums - moved :]
    dwg_ref, dwu_ref = outs[:2]
    ff = dwg_ref.shape[1]
    dw = lax.dot_general(
        x_ref[...], d_ref[...], (((0,), (0,)), ((), ())), preferred_element_type=jnp.float32
    )
    dwg_ref[...] = dw[:, :ff].astype(dwg_ref.dtype)
    dwu_ref[...] = dw[:, ff:].astype(dwu_ref.dtype)
    for k in range(sums):
        mine, came = rest[2 * k : 2 * k + 2]
        total = bf16(f32(mine[...]) + f32(came[...]))
        first, others = outs[2 + 2 * k], outs[3 + 2 * k]
        half, away = total.shape[1], total.shape[0] - 1
        early = half - first.shape[0]
        for j in range(away):
            others[j * half : (j + 1) * half, :] = total[1 + j]
        if early:
            others[away * half :, :] = total[0, :early]
        first[...] = total[0, early:]
    for k in range(moved):
        outs[2 + 2 * sums + k][...] = rest[2 * sums + k][...]


def dw_in(full, dgu, first, last, so_far=(), pairs=(), moved=()):
    _, tokens, d = full.shape
    ff = dgu.shape[1] // 2
    bd = tile_of(d, 256)
    n = last - first
    flat = [v for pair in pairs for v in pair[:2]]
    resident = 2 * dgu.size

    def along(v):
        lead = v.shape[:-1]
        return pl.BlockSpec((*lead, v.shape[-1] // n), lambda i: (*[0] * len(lead), i))

    extra = []
    for v, _, early in pairs:
        blocks, half, cols = v.shape
        for height in (half - early, (blocks - 1) * half + early):
            extra.append(jax.ShapeDtypeStruct((height, cols), v.dtype))
    extra += moved
    new = [jax.ShapeDtypeStruct((d, ff), full.dtype)] * 2 + [jax.ShapeDtypeStruct(v.shape, v.dtype) for v in extra]
    return pl.pallas_call(
        functools.partial(dw_in_kernel, len(pairs), len(moved)),
        grid=(n,),
        out_shape=new,
        in_specs=[
            pl.BlockSpec((pl.squeezed, tokens, bd), lambda i: (1, 0, i + first)),
            pl.BlockSpec(memory_space=pltpu.VMEM),
            *[along(v) for v in (*flat, *moved)],
            *[pl.BlockSpec(memory_space=pltpu.HBM)] * len(so_far),
        ],
        out_specs=[*[pl.BlockSpec((bd, ff), lambda i: (i + first, 0))] * 2, *[along(v) for v in extra]],
        input_output_aliases={2 + len(flat) + len(moved) + i: i for i in range(len(so_far))},
        compiler_params=pltpu.CompilerParams(vmem_limit_bytes=VMEM - resident - 65536),
        cost_estimate=pl.CostEstimate(
            flops=4 * tokens * n * bd * ff, bytes_accessed=2 * (tokens * n * bd + 2 * ff * (tokens + n * bd)), transcendentals=0
        ),
        name="dw_in",
    )(full, dgu, *flat, *moved, *so_far)


def f32(v):
    return v.astype(jnp.float32)


def bf16(v):
    return v.astype(jnp.bfloat16)


def finish_kernel(side, cut, *refs):
    ins, own, rest = refs[:12], refs[12:16], refs[16:]
    sum_ref, came_f, came_b, in_v, send_v, far_f, far_b, own_f, own_b, near_f, near_b, *sems = rest
    in_sem, send_sem, recv_sem, own_send, own_recv = sems
    rows, _ = sum_ref.shape[1:]
    half = rows // 2
    over = cut - half
    me = lax.axis_index("tp")
    at = (me // side, me % side)

    def neighbour(axis, sign):
        to = [at[0], at[1]]
        to[axis] = lax.rem(to[axis] + sign + side, side)
        return {"tp": to[0] * side + to[1]}

    barrier = pltpu.get_barrier_semaphore()
    for axis, sign in LINKS:
        pl.semaphore_signal(barrier, inc=1, device_id=neighbour(axis, sign), device_id_type=MESH)

    def late(r):
        return 1 + r

    early = ins[1].shape[0] - 3 * half

    def loads(h, j, r):
        copies = []
        for k in range(3):
            src, dst = ins[6 * h + 3 * r + k], in_v.at[h, j, r, k]
            if k != late(r):
                src = src.at[j]
            elif j > 0:
                src = src.at[pl.ds((j - 1) * half, half)]
            elif r == 0:
                src, dst = src.at[pl.ds(3 * half, early)], dst.at[pl.ds(0, early)]
            else:
                continue
            copies.append(pltpu.make_async_copy(src, dst, in_sem.at[h, j, r, k]))
        return copies

    def own_message(h, way):
        return pltpu.make_async_remote_copy(
            src_ref=own[2 * h + way],
            dst_ref=(own_f, own_b)[way].at[h],
            send_sem=own_send.at[h, way],
            recv_sem=own_recv.at[h, way],
            device_id=neighbour(h, 1 - 2 * way),
            device_id_type=MESH,
        )

    def message(h, step, way):
        top = way == 0 if step != 1 else way == 1
        block = pl.ds(0, cut) if top else pl.ds(cut, rows - cut)
        if step < 2:
            src = send_v.at[h, 2 if step == 0 else 1 + 2 * way, block]
        else:
            src = (near_f, near_b)[way].at[h]
        dst = (far_f, far_b)[way].at[h] if step == 0 else (came_f if top else came_b).at[h, step - 1]
        return pltpu.make_async_remote_copy(
            src_ref=src,
            dst_ref=dst,
            send_sem=send_sem.at[h, step, way],
            recv_sem=recv_sem.at[h, step, way],
            device_id=neighbour(1 - h, 1 - 2 * way),
            device_id_type=MESH,
        )

    def piece(h, j, r, wait=True):
        if wait:
            for c in loads(h, j, r):
                c.wait()
        return f32(in_v[h, j, r, 0]) + f32(in_v[h, j, r, 1]) + f32(in_v[h, j, r, 2])

    order = ((2, 0), (2, 1), (1, 1), (3, 0), (3, 1), (1, 0), (0, 0), (0, 1))
    for j, r in order:
        for h in range(2):
            for c in loads(h, j, r):
                c.start()
    pl.semaphore_wait(barrier, len(LINKS))
    for h in range(2):
        for way in range(2):
            own_message(h, way).start()

    def ready(h, j, r):
        send_v[h, j, r * half : (r + 1) * half, :] = bf16(piece(h, j, r))

    for h in range(2):
        ready(h, 2, 0)
        ready(h, 2, 1)
        message(h, 0, 0).start()
        message(h, 0, 1).start()
    for h in range(2):
        ready(h, 1, 1)
        message(h, 1, 0).start()
        ready(h, 3, 0)
        ready(h, 3, 1)
        message(h, 1, 1).start()
    for h in range(2):
        message(h, 0, 0).wait_recv()
        near_f[h, :half, :] = bf16(piece(h, 1, 0) + f32(far_f[h, :half, :]))
        near_f[h, half:, :] = bf16(piece(h, 1, 1, False)[:over] + f32(far_f[h, half:, :]))
        message(h, 2, 0).start()
        message(h, 0, 1).wait_recv()
        near_b[h] = bf16(piece(h, 3, 1, False)[over:] + f32(far_b[h]))
        message(h, 2, 1).start()
    for h in range(2):
        for r in range(2):
            for c in loads(h, 0, r):
                c.wait()
        kept = f32(in_v[h, 0, 0, 0]) + f32(in_v[h, 0, 0, 2])
        own_message(h, 0).wait_recv()
        sum_ref[h, :early, :] = kept[:early] + f32(in_v[h, 0, 0, 1, :early, :])
        sum_ref[h, early:half, :] = kept[early:] + f32(own_f[h])
        kept = f32(in_v[h, 0, 1, 0]) + f32(in_v[h, 0, 1, 1])
        own_message(h, 1).wait_recv()
        sum_ref[h, half:, :] = kept + f32(own_b[h])
    for step in (1, 2):
        for h in range(2):
            for way in range(2):
                message(h, step, way).wait_recv()
    for h in range(2):
        for way in range(2):
            own_message(h, way).wait_send()
            for step in range(3):
                message(h, step, way).wait_send()


def finish(side, cut, ins, own):
    _, half, cols = ins[0].shape
    rows = 2 * half
    hbm, vmem = pl.BlockSpec(memory_space=pltpu.HBM), pl.BlockSpec(memory_space=pltpu.VMEM)
    dtype = jnp.bfloat16
    mine, came_f, came_b = pl.pallas_call(
        functools.partial(finish_kernel, side, cut),
        out_shape=(
            pltpu.VMEM((2, rows, cols), jnp.float32),
            pltpu.VMEM((2, 2, cut, cols), dtype),
            pltpu.VMEM((2, 2, rows - cut, cols), dtype),
        ),
        in_specs=[hbm] * (len(ins) + len(own)),
        out_specs=(vmem,) * 3,
        scratch_shapes=[
            pltpu.VMEM((2, side, 2, 3, half, cols), dtype),
            pltpu.VMEM((2, side, rows, cols), dtype),
            pltpu.VMEM((2, cut, cols), dtype),
            pltpu.VMEM((2, rows - cut, cols), dtype),
            pltpu.VMEM((2, *own[0].shape), dtype),
            pltpu.VMEM((2, *own[1].shape), dtype),
            pltpu.VMEM((2, cut, cols), dtype),
            pltpu.VMEM((2, rows - cut, cols), dtype),
            pltpu.SemaphoreType.DMA((2, side, 2, 3)),
            pltpu.SemaphoreType.DMA((2, 3, 2)),
            pltpu.SemaphoreType.DMA((2, 3, 2)),
            pltpu.SemaphoreType.DMA((2, 2)),
            pltpu.SemaphoreType.DMA((2, 2)),
        ],
        compiler_params=pltpu.CompilerParams(
            collective_id=1, has_side_effects=True, vmem_limit_bytes=FINISH
        ),
        cost_estimate=pl.CostEstimate(
            flops=64 * half * cols, bytes_accessed=2 * 52 * half * cols, transcendentals=0
        ),
        name="finish_dx",
    )(*ins, *own)

    chunk = tile_of(cols, cols // 2)

    def last_sum(mine_ref, f_ref, b_ref, out_ref):
        i = pl.program_id(0)
        h, c = i // 2, pl.ds(pl.multiple_of(i % 2 * chunk, 128), chunk)
        for ref, block in ((f_ref, slice(0, cut)), (b_ref, slice(cut, rows))):
            out_ref[block, :] = bf16(mine_ref[h, block, c] + f32(ref[h, 0, :, c]) + f32(ref[h, 1, :, c]))

    return pl.pallas_call(
        last_sum,
        grid=(4,),
        out_shape=jax.ShapeDtypeStruct((rows, 2 * cols), dtype),
        in_specs=[vmem] * 3,
        out_specs=pl.BlockSpec((rows, chunk), lambda i: (0, i)),
        compiler_params=pltpu.CompilerParams(vmem_limit_bytes=16 * 1024 * 1024),
        cost_estimate=pl.CostEstimate(flops=8 * half * cols, bytes_accessed=16 * half * cols, transcendentals=0),
        name="last_sum",
    )(mine, came_f, came_b)


def solution(mesh):
    side = math.isqrt(mesh.shape["tp"])

    def hop(v, axis, sign):
        pairs = []
        for i in range(side * side):
            at = [i // side, i % side]
            at[axis] = (at[axis] + sign) % side
            pairs.append((i, at[0] * side + at[1]))
        return lax.ppermute(v, "tp", pairs)

    def device_step(x, dy, gate, up, w_gate, w_up, w_down):
        full, dgu, _, dw_down, *terms = gather(side, x, dy, gate, up, w_gate, w_up, w_down)
        t = [[terms[2 * (h * side + k) :][:2] for k in range(side)] for h in range(2)]
        dgu = pltpu.with_memory_space_constraint(dgu, pltpu.VMEM)
        blocks = x.shape[1] // tile_of(x.shape[1], 256)
        cuts = [0, blocks * 14 // 28, blocks * 18 // 28, blocks]
        far = [(hop(v[2][0], h, 1), hop(v[2][1], h, -1)) for h, v in enumerate(t)]
        raw = [(hop(v[1][1], h, 1), hop(v[3][0], h, -1)) for h, v in enumerate(t)]
        *dw, dw_down = dw_in(full, dgu, cuts[0], cuts[1], moved=[dw_down])
        half = x.shape[0] // 2
        pairs = [(v[1][0], f[0], 2 * half // 5) for v, f in zip(t, far)] + [(v[3][1], f[1], 0) for v, f in zip(t, far)]
        *dw, a0, a, b0, b, c0, c, d0, d = dw_in(full, dgu, cuts[1], cuts[2], dw, pairs)
        near = [(hop(up_, h, 1), hop(down, h, -1)) for h, (up_, down) in enumerate(((a, c), (b, d)))]
        dw = dw_in(full, dgu, cuts[2], cuts[3], dw)
        ins = []
        for v, r, n in zip(t, raw, near):
            ins += [v[0][0], n[0], r[1], v[0][1], r[0], n[1]]
        dx = finish(side, half + half // 5, ins, [a0, c0, b0, d0])
        return dx, *dw, dw_down

    rows, both, cols = P(("dp", "tp"), None), P("dp", "tp"), P(None, "tp")
    return jax.shard_map(
        device_step,
        mesh=mesh,
        in_specs=(rows, rows, both, both, cols, cols, P("tp", None)),
        out_specs=(rows, both, both, rows),
        check_vma=False,
    )
```
